32 devices in a mesh: sub: 8 (over y, x, core), mode: 4 (over z).
Axes of the slice: x: 2, y: 2, z: 4, core: 2. Of those that a mesh axis runs over, the one named last changes fastest.
Arguments:
- leaf_coords: bfloat16 [64, 768, 128], P('sub', 'mode'), may hold values from -6 to 6
- leaf_modes: bfloat16 [64, 128, 512], P('sub'), may hold values from -0.5 to 0.5
- constraint_modes: bfloat16 [64, 3, 256, 512], P('sub'), may hold values from -0.375 to 0.375
- sep_one: bfloat16 [768, 1024], P('mode', 'sub'), may hold values from -6 to 6
- sep_two: bfloat16 [768, 512], P('mode', 'sub'), may hold values from -6 to 6
- sep_three: bfloat16 [768, 256], P('mode', 'sub'), may hold values from -6 to 6
- cluster_rows: int32 [24, 512], P('sub'), may hold values from 0 to 32767, as said below
- operators: bfloat16 [24, 512, 384], P('sub'), may hold values from -0.25 to 0.25
- compliance: float32 [24, 384], P('sub'), may hold values from 0.05 to 0.5
- modal_weight: float32 [768], P('mode'), may hold values from 0.5 to 2
Outputs:
- stresses: float32 [24, 768, 384], P('sub', 'mode')
- strain_energy: float32 [1536], P(('sub', 'mode'))
The draws below stay inside these ranges and needn't reach their ends.
Inputs may be any that keep to these rules, and one draw needn't show every extreme that they name: cluster_rows[c, j] = s * 4096 + r names column r of the displacement columns of the leaves of sub index s (its leaves laid end to end). The clusters of sub index d read only from sub indices d - 2 to d + 2 taken around the axis, and at most 384 of their 1536 rows from any one of these indices; that most is reached for every d from one of the five.
All inputs are finite; a program needn't handle non-finite values.
Results may differ from the reference program's by a relative error of at most 0.0029.
Values may be sent and summed in bfloat16 or wider, within the bound.
No kernel may reach another device: no remote copies, remote signals or barrier semaphores. Data moves between devices by JAX's collectives and lax.ppermute only.
A program may use at most 64 MiB of HBM per device.

```python
import math
import jax
import jax.numpy as jnp
from jax import lax

M = 768
B = 256
R = 512
KL = 128
CW = 512
PTS = 64
LEAF_DEV = 8
CL_DEV = 3
SR = 384
LEAVES = 64
CLUSTERS = 24
DOFS = 4096
SEP_ONE = 1024
SEP_TWO = 512
SEP_THREE = 256


def draw_cluster_rows(key, part):
    key = jax.random.fold_in(key, 11)
    devices = CLUSTERS // CL_DEV
    slots = CL_DEV * CW
    first, second, third, fourth = jax.random.split(key, 4)
    swing = jax.random.randint(first, (devices, 2), -(slots // 16), slots // 16 + 1)
    middle = slots // 8 + slots // 16
    others = middle + jnp.stack([swing[:, 0], -swing[:, 0], swing[:, 1], -swing[:, 1]], axis=1)
    counts = jnp.concatenate([jnp.full((devices, 1), slots // 4, jnp.int32), others.astype(jnp.int32)], axis=1)
    scores = jax.random.randint(second, (devices, 5), 0, 1000) * 8 + jnp.arange(5, dtype=jnp.int32)[None, :]
    group_offset = jnp.argsort(scores, axis=1).astype(jnp.int32) - 2
    bounds = jnp.cumsum(counts, axis=1)
    position = jnp.arange(slots, dtype=jnp.int32)
    group = jnp.sum((position[None, :, None] >= bounds[:, None, :]).astype(jnp.int32), axis=2)
    slot_offset = jnp.take_along_axis(group_offset, group, axis=1)
    shuffle_keys = jax.random.randint(third, (devices, slots), 0, 1 << 14) * slots + position[None, :]
    shuffle = jnp.argsort(shuffle_keys, axis=1)
    slot_offset = jnp.take_along_axis(slot_offset, shuffle, axis=1)
    device_ids = jnp.arange(devices, dtype=jnp.int32)[:, None]
    source = (device_ids + slot_offset) % devices
    row_in = jax.random.randint(fourth, (devices, slots), 0, DOFS)
    flat = source * DOFS + row_in
    return flat.reshape(CLUSTERS, CW).astype(jnp.int32)


def level_of(key, shape, cuts, low, top_value):
    level, own = 1.0, jax.random.fold_in(key, 6)
    for dim, blocks in cuts:
        heights = jnp.exp(jax.random.uniform(jax.random.fold_in(own, dim), (blocks,), jnp.float32, low / len(cuts), top_value / len(cuts)))
        level = level * jnp.repeat(heights, shape[dim] // blocks).reshape([-1 if axis == dim else 1 for axis in range(len(shape))])
    return level


def noise(stream_key, shape, deviation, reach, cuts=(), held_as=jnp.bfloat16):
    result = deviation * jax.random.normal(stream_key, shape, jnp.float32)
    if cuts:
        result = result * level_of(stream_key, shape, cuts, -0.22, 0.18)
    return jnp.clip(result, -reach, reach).astype(held_as)


def setup_inputs(seed: int = 0) -> dict:
    keys = jax.random.split(jax.random.key(seed), 11)
    leaf_coords = noise(keys[0], (LEAVES, M, KL), 1.0, 6.0, ((0, 8), (1, 4)))
    leaf_modes = noise(keys[1], (LEAVES, KL, R), KL ** -0.5, 0.5, ((0, 8),))
    constraint_modes = noise(keys[2], (LEAVES, 3, B, R), B ** -0.5, 0.375, ((0, 8),))
    sep_one = noise(keys[3], (M, SEP_ONE), 1.0, 6.0, ((0, 4), (1, 8)))
    sep_two = noise(keys[4], (M, SEP_TWO), 1.0, 6.0, ((0, 4), (1, 8)))
    sep_three = noise(keys[5], (M, SEP_THREE), 1.0, 6.0, ((0, 4), (1, 8)))
    cluster_rows = draw_cluster_rows(jax.random.fold_in(keys[10], 71), 0)
    operators = noise(keys[7], (CLUSTERS, CW, SR), CW ** -0.5, 0.25, ((0, 8),))
    compliance = jnp.clip(jnp.exp(math.log(0.5) - 2.3025851 * jax.random.uniform(keys[8], (CLUSTERS, SR), jnp.float32) ** level_of(keys[8], (CLUSTERS, SR), ((0, 8),), -0.2, 0.2)), 0.05, 0.5)
    modal_weight = jnp.clip(jnp.exp(math.log(2.0) - 1.3862944 * jax.random.uniform(keys[9], (M,), jnp.float32) ** level_of(keys[9], (M,), ((0, 4),), -0.2, 0.2)), 0.5, 2.0)
    return dict(leaf_coords=leaf_coords, leaf_modes=leaf_modes, constraint_modes=constraint_modes, sep_one=sep_one, sep_two=sep_two, sep_three=sep_three, cluster_rows=cluster_rows, operators=operators, compliance=compliance, modal_weight=modal_weight)


def reference(leaf_coords, leaf_modes, constraint_modes, sep_one, sep_two, sep_three, cluster_rows, operators, compliance, modal_weight):
    separators = (sep_one, sep_two, sep_three)

    def one_leaf(leaf):
        device = leaf // LEAF_DEV
        total = jnp.dot(leaf_coords[leaf].astype(jnp.float32), leaf_modes[leaf].astype(jnp.float32), preferred_element_type=jnp.float32)
        for level in range(3):
            node = (device >> (level + 1)).astype(jnp.int32)
            block = lax.dynamic_slice(separators[level], (jnp.int32(0), (node * B).astype(jnp.int32)), (M, B))
            total = total + jnp.dot(block.astype(jnp.float32), constraint_modes[leaf, level].astype(jnp.float32), preferred_element_type=jnp.float32)
        return total.astype(jnp.bfloat16)

    displaced = lax.map(one_leaf, jnp.arange(LEAVES, dtype=jnp.int32))
    flat = jnp.transpose(displaced, (1, 0, 2)).reshape(M, LEAVES * R)

    def one_cluster(inputs):
        row_ids, operator, weights = inputs
        gathered = jnp.take(flat, row_ids, axis=1)
        stress = jnp.dot(gathered.astype(jnp.float32), operator.astype(jnp.float32), preferred_element_type=jnp.float32)
        weighted = jnp.sum(modal_weight[:, None] * stress * stress, axis=0) * weights
        energy = jnp.sum(weighted.reshape(6, PTS), axis=0) * (0.5 / M)
        return stress, energy

    stresses, energies = lax.map(one_cluster, (cluster_rows, operators, compliance))
    return stresses, energies.reshape(CLUSTERS * PTS)
```

```python
import jax
import jax.numpy as jnp
from jax import lax
from jax.experimental import pallas as pl
from jax.experimental.pallas import tpu as pltpu
from jax.sharding import PartitionSpec as P

VMEM = pltpu.VMEM
SMEM = pltpu.SMEM
OFFSETS = (-2, -1, 0, 1, 2)
REMOTE = (-2, -1, 1, 2)
F32 = jnp.float32
BF16 = jnp.bfloat16


def params(mib):
    return pltpu.CompilerParams(vmem_limit_bytes=mib * 1024 * 1024)


def cost(flops, nbytes):
    return pl.CostEstimate(flops=flops, bytes_accessed=nbytes, transcendentals=0)


def vmem_specs(count):
    return [pl.BlockSpec(memory_space=VMEM)] * count


def shift_by(value, axis, by):
    peers = lax.axis_size(axis)
    return lax.ppermute(value, axis, [(i, (i + by) % peers) for i in range(peers)])


def swap_with(value, axis, mask):
    return lax.ppermute(value, axis, [(i, i ^ mask) for i in range(lax.axis_size(axis))])


def pack_kernel(one_ref, two_ref, three_ref, out_ref):
    wide = one_ref.shape[1]
    mid = two_ref.shape[0]
    out_ref[:wide, :] = one_ref[...].astype(F32).T.astype(BF16)
    out_ref[wide : wide + mid, :] = two_ref[...]
    out_ref[wide + mid :, :] = three_ref[...]


def one_hot(target, first, rows):
    local = target - first
    local = jnp.where((local >= 0) & (local < rows), local, -1).astype(F32).astype(BF16)
    ids = lax.broadcasted_iota(jnp.int32, (rows, target.shape[1]), 0).astype(F32).astype(BF16)
    hit = ids == jnp.broadcast_to(local, ids.shape)
    return jnp.where(hit, jnp.ones((), BF16), jnp.zeros((), BF16))


def index_kernel(sub_count, dof_count, capacity, me_ref, rows_ref, key_ref, wanted_ref):
    clusters, width = rows_ref.shape
    row = rows_ref[...]
    source = lax.div(row, jnp.int32(dof_count))
    local = row - source * dof_count
    distance = source - me_ref[0]
    distance = jnp.where(distance < 0, distance + sub_count, distance)
    offset = jnp.where(distance > sub_count // 2, distance - sub_count, distance)
    before = lax.broadcasted_iota(jnp.int32, (width, width), 0)
    after = lax.broadcasted_iota(jnp.int32, (width, width), 1)
    upper = jnp.where(before <= after, 1.0, 0.0).astype(BF16)
    key = jnp.zeros((clusters, width), F32)
    for number, each in enumerate(OFFSETS):
        mask = jnp.where(offset == each, 1.0, 0.0)
        count = jnp.dot(mask.astype(BF16), upper, preferred_element_type=F32)
        carried = jnp.full((1, 1), float(number * capacity - 1), F32)
        placed = []
        for cluster in range(clusters):
            placed.append(count[cluster : cluster + 1, :] + carried)
            carried = carried + count[cluster : cluster + 1, width - 1 : width]
        key = key + mask * jnp.concatenate(placed, axis=0)
    key = key.astype(jnp.int32)
    key_ref[...] = key
    high = lax.div(local, jnp.int32(64))
    low = local - high * 64
    tile = 128
    for part in range(len(OFFSETS) * capacity // tile):
        total = jnp.zeros((2, tile), F32)
        for cluster in range(clusters):
            pick = one_hot(key[cluster : cluster + 1, :], part * tile, tile)
            values = jnp.concatenate(
                [high[cluster : cluster + 1, :], low[cluster : cluster + 1, :]], axis=0
            )
            total = total + lax.dot_general(
                values.astype(F32).astype(BF16),
                pick,
                (((1,), (1,)), ((), ())),
                preferred_element_type=F32,
            )
        answer = (total[0:1, :] * 64.0 + total[1:2, :]).astype(jnp.int32)
        wanted_ref[:, part * tile : (part + 1) * tile] = answer


def displace_kernel(
    me_ref,
    coords_ref,
    modes_ref,
    couple_ref,
    mine_ref,
    pair_ref,
    next_ref,
    far_ref,
    diag_ref,
    *rest,
):
    flows = len(rest) - 3 >> 1
    wanted = rest[:flows]
    outs = rest[flows : 2 * flows]
    anc_t, disp, total = rest[2 * flows :]
    leaves, modes, inner = coords_ref.shape
    width = modes_ref.shape[2]
    block = couple_ref.shape[2]
    me = me_ref[0]
    core = lax.rem(me, 2)
    chip = lax.rem(lax.div(me, 2), 4)
    half, quarter, eighth = block // 2, block // 4, block // 8

    def put(level, at, rows, value):
        anc_t[pl.ds(pl.multiple_of(level * block + at * rows, rows), rows), :] = value

    for which, ref in ((core, mine_ref), (1 - core, pair_ref)):
        put(0, which, half, ref[:half, :])
        put(1, 2 * lax.rem(chip, 2) + which, quarter, ref[half : half + quarter, :])
        put(2, 2 * chip + which, eighth, ref[half + quarter :, :])
    two = 2 * quarter
    near = chip + 1 - 2 * lax.rem(chip, 2)
    across = lax.rem(chip + 2, 4)
    diagonal = near + 2 - 4 * lax.div(near, 2)
    put(1, 1 - lax.rem(chip, 2), two, next_ref[:two, :])
    put(2, near, 2 * eighth, next_ref[two:, :])
    put(2, across, 2 * eighth, far_ref[...])
    put(2, diagonal, 2 * eighth, diag_ref[...])
    anc = anc_t[...].astype(F32).T.astype(BF16)
    for leaf in range(leaves):
        value = jnp.dot(coords_ref[leaf], modes_ref[leaf], preferred_element_type=F32)
        for level in range(couple_ref.shape[1]):
            value = value + jnp.dot(
                anc[:, level * block : (level + 1) * block],
                couple_ref[leaf, level],
                preferred_element_type=F32,
            )
        disp[:, leaf * width : (leaf + 1) * width] = value.astype(BF16)
    tile = 256
    for flow in range(flows):
        total[...] = jnp.zeros_like(total)
        want = wanted[flow][...]

        def step(part, carry, want=want):
            at = pl.multiple_of(part * tile, tile)
            total[...] += jnp.dot(
                disp[:, pl.ds(at, tile)], one_hot(want, at, tile), preferred_element_type=F32
            )
            return carry

        lax.fori_loop(0, leaves * width // tile, step, 0, unroll=4)
        outs[flow][...] = total[...].astype(BF16)


def permute_kernel(key_ref, operators_ref, out_ref):
    clusters, width, rows = operators_ref.shape
    tile = 128
    for part in range(out_ref.shape[0] // tile):
        for cluster in range(clusters):
            pick = one_hot(key_ref[cluster : cluster + 1, :], part * tile, tile)
            moved = jnp.dot(pick, operators_ref[cluster], preferred_element_type=F32)
            out_ref[
                part * tile : (part + 1) * tile, cluster * rows : (cluster + 1) * rows
            ] = moved.astype(BF16)


def stress_kernel(capacity, scale, weight_ref, compliance_ref, moved_ref, *rest):
    count = len(OFFSETS)
    arrived = rest[:count]
    stress_ref, energy_ref = rest[count:]
    clusters, modes, rows = stress_ref.shape
    points = energy_ref.shape[1]
    weight = weight_ref[...]
    for cluster in range(clusters):
        value = jnp.zeros((modes, rows), F32)
        for number in range(count):
            value = value + jnp.dot(
                arrived[number][...],
                moved_ref[
                    number * capacity : (number + 1) * capacity,
                    cluster * rows : (cluster + 1) * rows,
                ],
                preferred_element_type=F32,
            )
        stress_ref[cluster] = value
        square = jnp.sum(value * value * weight, axis=0, keepdims=True)
        square = square * compliance_ref[cluster : cluster + 1, :]
        term = square[:, :points]
        for part in range(1, rows // points):
            term = term + square[:, part * points : (part + 1) * points]
        energy_ref[cluster : cluster + 1, :] = term * scale


def shards(
    leaf_coords,
    leaf_modes,
    constraint_modes,
    sep_one,
    sep_two,
    sep_three,
    cluster_rows,
    operators,
    compliance,
    modal_weight,
):
    sub_count = lax.axis_size("sub")
    mode_count = lax.axis_size("mode")
    me = lax.axis_index("sub").astype(jnp.int32).reshape(1)
    leaves, modes, inner = leaf_coords.shape
    width = leaf_modes.shape[2]
    dof_count = leaves * width
    levels, block = constraint_modes.shape[1:3]
    clusters, slots = cluster_rows.shape
    rows = operators.shape[2]
    capacity = clusters * slots // 4
    count = len(OFFSETS)
    smem = pl.BlockSpec(memory_space=SMEM)
    vmem = pl.BlockSpec(memory_space=VMEM)

    held = sep_one.shape[1] + sep_two.shape[1] + sep_three.shape[1]
    mine = pl.pallas_call(
        pack_kernel,
        out_shape=jax.ShapeDtypeStruct((held, modes), BF16),
        in_specs=vmem_specs(3),
        out_specs=vmem,
        compiler_params=params(4),
        cost_estimate=cost(10000000, 300000),
        name="pack",
    )(sep_one, sep_two.T, sep_three.T)
    pair = swap_with(mine, "sub", 1)

    key, wanted = pl.pallas_call(
        lambda *refs: index_kernel(sub_count, dof_count, capacity, *refs),
        out_shape=(
            jax.ShapeDtypeStruct((clusters, slots), jnp.int32),
            jax.ShapeDtypeStruct((1, count * capacity), jnp.int32),
        ),
        in_specs=[smem, vmem],
        out_specs=(vmem, vmem),
        compiler_params=params(8),
        cost_estimate=cost(1500000000, 300000),
        name="index",
    )(me, cluster_rows)
    lists = []
    for number, offset in enumerate(OFFSETS):
        piece = wanted[:, number * capacity : (number + 1) * capacity]
        lists.append(shift_by(piece, "sub", offset) if offset else piece)

    odd = lax.rem(me[0], 2) == 1
    first = jnp.where(odd, pair, mine)
    second = jnp.where(odd, mine, pair)
    half, quarter = sep_one.shape[1], sep_two.shape[1]
    both = jnp.concatenate(
        [
            first[half : half + quarter],
            second[half : half + quarter],
            first[half + quarter :],
            second[half + quarter :],
        ],
        axis=0,
    )
    near = swap_with(both, "sub", 2)
    far = swap_with(both[2 * quarter :], "sub", 4)
    diag = swap_with(both[2 * quarter :], "sub", 6)

    picked = pl.pallas_call(
        displace_kernel,
        out_shape=(jax.ShapeDtypeStruct((modes, capacity), BF16),) * count,
        in_specs=[smem] + vmem_specs(8 + count),
        out_specs=(vmem,) * count,
        scratch_shapes=[
            VMEM((levels * block, modes), BF16),
            VMEM((modes, dof_count), BF16),
            VMEM((modes, capacity), F32),
        ],
        compiler_params=params(24),
        cost_estimate=cost(8000000000, 9000000),
        name="displace",
    )(me, leaf_coords, leaf_modes, constraint_modes, mine, pair, near, far, diag, *lists)

    arrived = [
        shift_by(piece, "sub", -offset) if offset else piece
        for piece, offset in zip(picked, OFFSETS)
    ]
    moved = pl.pallas_call(
        permute_kernel,
        out_shape=jax.ShapeDtypeStruct((count * capacity, clusters * rows), BF16),
        in_specs=vmem_specs(2),
        out_specs=vmem,
        compiler_params=params(16),
        cost_estimate=cost(6000000000, 6000000),
        name="permute",
    )(key, operators)

    points = rows // 6
    stresses, energy = pl.pallas_call(
        lambda *refs: stress_kernel(capacity, 0.5 / (modes * mode_count), *refs),
        out_shape=(
            jax.ShapeDtypeStruct((clusters, modes, rows), F32),
            jax.ShapeDtypeStruct((clusters, points), F32),
        ),
        in_specs=vmem_specs(3 + count),
        out_specs=(vmem, vmem),
        compiler_params=params(16),
        cost_estimate=cost(1000000000, 6000000),
        name="stress",
    )(modal_weight.reshape(modes, 1), compliance, moved, *arrived)

    total = energy
    for step in range(1, mode_count):
        total = total + shift_by(energy, "mode", step)
    share = clusters * points // mode_count
    strain_energy = lax.dynamic_slice(
        total.reshape(-1), (lax.axis_index("mode") * share,), (share,)
    )
    return (stresses, strain_energy)


def solution(mesh):
    return jax.shard_map(
        shards,
        mesh=mesh,
        in_specs=(
            P("sub", "mode", None),
            P("sub", None, None),
            P("sub", None, None, None),
            P("mode", "sub"),
            P("mode", "sub"),
            P("mode", "sub"),
            P("sub", None),
            P("sub", None, None),
            P("sub", None),
            P("mode"),
        ),
        out_specs=(P("sub", "mode", None), P(("sub", "mode"))),
        check_vma=False,
    )
```

```python
import jax
import jax.numpy as jnp
from jax import lax
from jax.experimental import pallas as pl
from jax.experimental.pallas import tpu as pltpu
from jax.sharding import PartitionSpec as P

VMEM = pltpu.VMEM
F32 = jnp.float32
BF16 = jnp.bfloat16
I32 = jnp.int32
BASE = 64
GROUP = 4

PLUS, MINUS, PAIR, OWN, CROSS = range(5)


def shift_by(value, axis, by):
    peers = lax.axis_size(axis)
    return lax.ppermute(value, axis, [(i, (i + by) % peers) for i in range(peers)])


def swap_with(value, axis, mask):
    return lax.ppermute(value, axis, [(i, i ^ mask) for i in range(lax.axis_size(axis))])


def swap_across(value, axis):
    peers = lax.axis_size(axis)
    return lax.ppermute(
        value, axis, [(i, (i + 2 * (i % 2) - 1) % peers) for i in range(peers)]
    )


def call(kernel, name, inputs, outputs, mib, flops, specs=None, scratch=()):
    vmem = pl.BlockSpec(memory_space=VMEM)
    many = isinstance(outputs, tuple)
    nbytes = sum(x.size * x.dtype.itemsize for x in inputs)
    return pl.pallas_call(
        kernel,
        out_shape=outputs,
        in_specs=specs or [vmem] * len(inputs),
        out_specs=(vmem,) * len(outputs) if many else vmem,
        scratch_shapes=list(scratch),
        compiler_params=pltpu.CompilerParams(vmem_limit_bytes=mib * 1024 * 1024),
        cost_estimate=pl.CostEstimate(flops=flops, bytes_accessed=nbytes, transcendentals=0),
        name=name,
    )(*inputs)


def one_hot(target, first, rows):
    local = target - first
    local = jnp.where((local >= 0) & (local < rows), local, -1).astype(F32).astype(BF16)
    ids = lax.broadcasted_iota(I32, (rows, target.shape[1]), 0).astype(F32).astype(BF16)
    hit = ids == jnp.broadcast_to(local, ids.shape)
    return jnp.where(hit, jnp.ones((), BF16), jnp.zeros((), BF16))


def list_rows(key, digits, group, capacity):
    clusters = len(digits)
    parts = []
    tile = 128
    for part in range(capacity // tile):
        total = jnp.zeros((2, tile), F32)
        for cluster in range(clusters):
            pick = one_hot(key[cluster : cluster + 1, :], group * capacity + part * tile, tile)
            total = total + lax.dot_general(
                digits[cluster], pick, (((1,), (1,)), ((), ())), preferred_element_type=F32
            )
        parts.append(total)
    return [part[0:1, :] for part in parts] + [part[1:2, :] for part in parts]


def digit_rows(local, clusters):
    high = lax.div(local, jnp.int32(BASE))
    low = local - high * BASE
    return [
        jnp.concatenate([high[c : c + 1, :], low[c : c + 1, :]], axis=0).astype(F32).astype(BF16)
        for c in range(clusters)
    ]


def filled(rows, count):
    lanes = rows[0].shape[1]
    rest = count - sum(row.shape[0] for row in rows)
    return jnp.concatenate(rows + [jnp.zeros((rest, lanes), F32)], axis=0)


def unpacked(block, start, capacity):
    parts = capacity // 128
    block = block.astype(F32)
    high = [block[start + i : start + i + 1, :] for i in range(parts)]
    low = [block[start + parts + i : start + parts + i + 1, :] for i in range(parts)]
    wanted = jnp.concatenate(high, axis=1) * float(BASE) + jnp.concatenate(low, axis=1)
    return wanted.astype(I32)


def list_height(capacity, lists):
    return (2 * capacity // 128 * lists + 15) // 16 * 16


def prep_kernel(
    sub_count,
    dof_count,
    capacity,
    me_ref,
    one_hbm,
    two_hbm,
    three_hbm,
    rows_hbm,
    out_ref,
    key_ref,
    local_ref,
    one_ref,
    two_ref,
    three_ref,
    rows_ref,
    sems,
):
    moves = [
        pltpu.make_async_copy(source, target, sems.at[number])
        for number, (source, target) in enumerate(
            (
                (rows_hbm, rows_ref),
                (one_hbm, one_ref),
                (two_hbm, two_ref),
                (three_hbm, three_ref),
            )
        )
    ]
    for move in moves:
        move.start()
    clusters, width = rows_ref.shape
    before = lax.broadcasted_iota(I32, (width, width), 0)
    after = lax.broadcasted_iota(I32, (width, width), 1)
    upper = jnp.where(before <= after, 1.0, 0.0).astype(BF16)
    moves[0].wait()
    row = rows_ref[...]
    me = me_ref[0]
    odd = lax.rem(me, 2)
    source = lax.div(row, jnp.int32(dof_count))
    local = row - source * dof_count
    distance = source - me
    distance = jnp.where(distance < 0, distance + sub_count, distance)
    offset = jnp.where(distance > sub_count // 2, distance - sub_count, distance)
    cross = 2 * odd - 1
    masks = [
        jnp.where(offset == each, 1.0, 0.0) for each in (2, -2, -cross, 0, cross)
    ]
    key = jnp.zeros((clusters, width), F32)
    for number, mask in enumerate(masks):
        count = jnp.dot(mask.astype(BF16), upper, preferred_element_type=F32)
        carried = jnp.full((1, 1), float(number * capacity - 1), F32)
        placed = []
        for cluster in range(clusters):
            placed.append(count[cluster : cluster + 1, :] + carried)
            carried = carried + count[cluster : cluster + 1, width - 1 : width]
        key = key + mask * jnp.concatenate(placed, axis=0)
    key = key.astype(I32)
    key_ref[...] = key
    local_ref[...] = local
    digits = digit_rows(local, clusters)
    rows = list_rows(key, digits, PAIR, capacity) + list_rows(key, digits, CROSS, capacity)
    wide, mid, small = one_ref.shape[1], two_ref.shape[0], three_ref.shape[0]
    head = wide + mid + small
    tail = list_height(capacity, 2)
    out_ref[head : head + tail, :] = jnp.zeros((tail, out_ref.shape[1]), BF16)
    out_ref[head : head + tail, :128] = filled(rows, tail).astype(BF16)
    for move in moves[1:]:
        move.wait()
    out_ref[:wide, :] = one_ref[...].astype(F32).T.astype(BF16)
    out_ref[wide : wide + mid, :] = two_ref[...]
    out_ref[wide + mid : head, :] = three_ref[...]


def lists_kernel(capacity, key_ref, local_ref, out_ref):
    clusters = key_ref.shape[0]
    key = key_ref[...]
    digits = digit_rows(local_ref[...], clusters)
    height = list_height(capacity, 1)
    for number, group in enumerate((PLUS, MINUS, OWN)):
        rows = list_rows(key, digits, group, capacity)
        out_ref[number * height : (number + 1) * height, :] = filled(rows, height).astype(BF16)


def relay_kernel(
    capacity, half, quarter, eighth, me_ref, mine_ref, pair_ref, lists_ref, up_ref, down_ref, far_ref
):
    odd = lax.rem(me_ref[0], 2)
    two = half
    three = half + quarter
    head = three + eighth
    tall = 2 * capacity // 128

    def put(ref, at, rows, which, value):
        ref[pl.ds(pl.multiple_of(at + which * rows, rows), rows), :] = value

    for which, ref in ((odd, mine_ref), (1 - odd, pair_ref)):
        for target in (up_ref, down_ref):
            put(target, 0, quarter, which, ref[two:three, :])
            put(target, 2 * quarter, eighth, which, ref[three:head, :])
        put(far_ref, 0, eighth, which, ref[three:head, :])
    base = 2 * (quarter + eighth)
    tail = up_ref.shape[0] - base
    relayed = pair_ref[head : head + list_height(capacity, 2), :128].astype(F32)
    relayed = relayed[tall : 2 * tall, :]
    height = list_height(capacity, 1)
    for target, number in ((up_ref, 0), (down_ref, 1)):
        own = lists_ref[number * height : (number + 1) * height, :].astype(F32)[:tall, :]
        target[base:, :] = jnp.zeros((tail, target.shape[1]), BF16)
        target[base:, :128] = filled([own, relayed], tail).astype(BF16)


def direct_kernel(coords_ref, modes_ref, out_ref):
    leaves = coords_ref.shape[0]
    width = modes_ref.shape[2]
    for leaf in range(leaves):
        out_ref[:, leaf * width : (leaf + 1) * width] = jnp.dot(
            coords_ref[leaf], modes_ref[leaf], preferred_element_type=F32
        )


def gathered(disp_ref, wanted):
    depth = 256
    total = None
    for at in range(0, disp_ref.shape[1], depth):
        part = jnp.dot(
            disp_ref[:, at : at + depth], one_hot(wanted, at, depth), preferred_element_type=F32
        )
        total = part if total is None else total + part
    return total.astype(BF16)


def displace_kernel(
    capacity,
    shifts,
    wraps,
    me_ref,
    direct_ref,
    couple_ref,
    mine_ref,
    pair_ref,
    lists_ref,
    *rest,
):
    arrays = rest[: len(shifts)]
    disp_ref, wanted_ref, cross_ref, anc_t = rest[len(shifts) :]
    leaves, levels, block, width = couple_ref.shape
    me = me_ref[0]
    odd = lax.rem(me, 2)
    chip = lax.rem(lax.div(me, 2), GROUP)
    half, quarter, eighth = block // 2, block // 4, block // 8

    def put(level, at, rows, value):
        anc_t[pl.ds(pl.multiple_of(level * block + at * rows, rows), rows), :] = value

    for which, ref in ((odd, mine_ref), (1 - odd, pair_ref)):
        put(0, which, half, ref[:half, :])
        put(1, 2 * lax.rem(chip, 2) + which, quarter, ref[half : half + quarter, :])
        put(2, 2 * chip + which, eighth, ref[half + quarter : half + quarter + eighth, :])
    two = 2 * quarter
    up, down = arrays[0], arrays[1]
    beside = 1 - lax.rem(chip, 2)
    low = lax.rem(chip, 2) == 0
    put(1, beside, two, jnp.where(low, down[:two, :], up[:two, :]))
    for shift, ref in zip(shifts, arrays):
        at = two if ref.shape[0] > 2 * eighth else 0
        place = chip - shift
        if wraps:
            put(2, lax.rem(place + GROUP, GROUP), 2 * eighth, ref[at : at + 2 * eighth, :])
        else:

            @pl.when((place >= 0) & (place < GROUP))
            def _(place=place, ref=ref, at=at):
                put(2, place, 2 * eighth, ref[at : at + 2 * eighth, :])

    anc = anc_t[...].astype(F32).T.astype(BF16)
    for leaf in range(leaves):
        value = direct_ref[:, leaf * width : (leaf + 1) * width]
        for level in range(levels):
            value = value + jnp.dot(
                anc[:, level * block : (level + 1) * block],
                couple_ref[leaf, level],
                preferred_element_type=F32,
            )
        disp_ref[:, leaf * width : (leaf + 1) * width] = value.astype(BF16)

    tall = 2 * capacity // 128
    height = list_height(capacity, 1)
    base = two + 2 * eighth
    up_lists, down_lists = up[base:, :128], down[base:, :128]
    head = half + quarter + eighth
    pair_lists = pair_ref[head : head + list_height(capacity, 2), :128]
    wanted_ref[:, :capacity] = unpacked(up_lists, 0, capacity)
    wanted_ref[:, capacity : 2 * capacity] = unpacked(down_lists, 0, capacity)
    wanted_ref[:, 2 * capacity : 3 * capacity] = unpacked(pair_lists, 0, capacity)
    wanted_ref[:, 3 * capacity :] = unpacked(
        lists_ref[2 * height : 3 * height, :], 0, capacity
    )
    across = jnp.where(
        odd == 1, unpacked(down_lists, tall, capacity), unpacked(up_lists, tall, capacity)
    )
    cross_ref[...] = gathered(disp_ref, across)


def gather_kernel(capacity, first, disp_ref, wanted_ref, left_ref, right_ref):
    both = gathered(
        disp_ref, wanted_ref[:, first * capacity : (first + 2) * capacity]
    )
    left_ref[...] = both[:, :capacity]
    right_ref[...] = both[:, capacity:]


def permute_kernel(first, key_ref, operators_ref, out_ref):
    clusters, width, rows = operators_ref.shape
    tile = 384
    for part in range(out_ref.shape[0] // tile):
        for cluster in range(clusters):
            for at in range(0, tile, 128):
                pick = one_hot(
                    key_ref[cluster : cluster + 1, :], first + part * tile + at, 128
                )
                moved = jnp.dot(pick, operators_ref[cluster], preferred_element_type=F32)
                start = part * tile + at
                out_ref[start : start + 128, cluster * rows : (cluster + 1) * rows] = (
                    moved.astype(BF16)
                )


def early_kernel(capacity, moved_ref, pair_ref, own_ref, cross_ref, out_ref):
    clusters, modes, rows = out_ref.shape
    for cluster in range(clusters):
        value = None
        for number, ref in enumerate((pair_ref, own_ref, cross_ref)):
            part = jnp.dot(
                ref[...],
                moved_ref[
                    number * capacity : (number + 1) * capacity,
                    cluster * rows : (cluster + 1) * rows,
                ],
                preferred_element_type=F32,
            )
            value = part if value is None else value + part
        out_ref[cluster] = value


def late_kernel(
    capacity,
    scale,
    weight_ref,
    compliance_ref,
    early_ref,
    moved_ref,
    plus_ref,
    minus_ref,
    stress_ref,
    energy_ref,
):
    clusters, modes, rows = stress_ref.shape
    points = energy_ref.shape[1]
    weight = weight_ref[...]
    for cluster in range(clusters):
        value = early_ref[cluster]
        for number, ref in enumerate((plus_ref, minus_ref)):
            value = value + jnp.dot(
                ref[...],
                moved_ref[
                    number * capacity : (number + 1) * capacity,
                    cluster * rows : (cluster + 1) * rows,
                ],
                preferred_element_type=F32,
            )
        stress_ref[cluster] = value
        square = jnp.sum(value * value * weight, axis=0, keepdims=True)
        square = square * compliance_ref[cluster : cluster + 1, :]
        term = square[:, :points]
        for part in range(1, rows // points):
            term = term + square[:, part * points : (part + 1) * points]
        energy_ref[cluster : cluster + 1, :] = term * scale


def store_kernel(source_ref, target_hbm, sem):
    move = pltpu.make_async_copy(source_ref, target_hbm, sem)
    move.start()
    move.wait()


def share_kernel(at_ref, mine_ref, other_ref, out_ref):
    clusters, points = mine_ref.shape
    total = mine_ref[...] + other_ref[...]
    row = [total[c : c + 1, :] for c in range(clusters)]
    lanes = (clusters * points + 127) // 128 * 128
    if lanes > clusters * points:
        row.append(jnp.zeros((1, lanes - clusters * points), F32))
    flat = jnp.broadcast_to(jnp.concatenate(row, axis=1), (8, lanes))
    share = out_ref.shape[1]
    moved = pltpu.roll(flat, lanes - at_ref[0] * share, 1)
    out_ref[...] = moved[0:1, :share]


def shards(
    leaf_coords,
    leaf_modes,
    constraint_modes,
    sep_one,
    sep_two,
    sep_three,
    cluster_rows,
    operators,
    compliance,
    modal_weight,
):
    sub_count = lax.axis_size("sub")
    mode_count = lax.axis_size("mode")
    me = lax.axis_index("sub").astype(I32).reshape(1)
    leaves, modes, inner = leaf_coords.shape
    width = leaf_modes.shape[2]
    dof_count = leaves * width
    levels, block = constraint_modes.shape[1:3]
    clusters, slots = cluster_rows.shape
    rows = operators.shape[2]
    points = rows // 6
    capacity = clusters * slots // 4
    smem = pl.BlockSpec(memory_space=pltpu.SMEM)
    vmem = pl.BlockSpec(memory_space=VMEM)
    hbm = pl.BlockSpec(memory_space=pltpu.HBM)
    array = jax.ShapeDtypeStruct
    half, quarter, eighth = sep_one.shape[1], sep_two.shape[1], sep_three.shape[1]

    held = half + quarter + eighth + list_height(capacity, 2)
    mine, key, local = call(
        lambda *refs: prep_kernel(sub_count, dof_count, capacity, *refs),
        "prep",
        (me, sep_one, sep_two.T, sep_three.T, cluster_rows),
        (
            array((held, modes), BF16),
            array((clusters, slots), I32),
            array((clusters, slots), I32),
        ),
        8,
        1000000000,
        [smem, hbm, hbm, hbm, hbm],
        [
            VMEM((modes, half), BF16),
            VMEM((quarter, modes), BF16),
            VMEM((eighth, modes), BF16),
            VMEM((clusters, slots), I32),
            pltpu.SemaphoreType.DMA((4,)),
        ],
    )
    pair = swap_with(mine, "sub", 1)
    lists = call(
        lambda *refs: lists_kernel(capacity, *refs),
        "lists",
        (key, local),
        array((3 * list_height(capacity, 1), 128), BF16),
        8,
        1000000000,
    )
    sent = 2 * (quarter + eighth)
    up, down, far = call(
        lambda *refs: relay_kernel(capacity, half, quarter, eighth, *refs),
        "relay",
        (me, mine, pair, lists),
        (
            array((sent + list_height(capacity, 2), modes), BF16),
            array((sent + list_height(capacity, 2), modes), BF16),
            array((2 * eighth, modes), BF16),
        ),
        4,
        10000000,
        [smem, vmem, vmem, vmem],
    )
    wraps = sub_count == 2 * GROUP
    shifts = (1, -1, 2) if wraps else (1, -1, 2, -2, 3, -3)
    arrays = [
        shift_by({1: up, -1: down}.get(shift, far), "sub", 2 * shift) for shift in shifts
    ]
    direct = call(
        direct_kernel,
        "direct",
        (leaf_coords, leaf_modes),
        array((modes, dof_count), F32),
        4,
        1500000000,
    )
    disp, wanted, cross = call(
        lambda *refs: displace_kernel(capacity, shifts, wraps, *refs),
        "displace",
        (me, direct, constraint_modes, mine, pair, lists, *arrays),
        (
            array((modes, dof_count), BF16),
            array((1, 4 * capacity), I32),
            array((modes, capacity), BF16),
        ),
        12,
        3000000000,
        [smem] + [vmem] * (5 + len(arrays)),
        [VMEM((levels * block, modes), BF16)],
    )
    cross = swap_across(cross, "sub")
    flow = array((modes, capacity), BF16)
    plus, minus = call(
        lambda *refs: gather_kernel(capacity, 0, *refs),
        "gather_far",
        (disp, wanted),
        (flow, flow),
        12,
        2000000000,
    )
    plus = shift_by(plus, "sub", -2)
    minus = shift_by(minus, "sub", 2)
    other, own = call(
        lambda *refs: gather_kernel(capacity, 2, *refs),
        "gather_near",
        (disp, wanted),
        (flow, flow),
        12,
        2000000000,
    )
    other = swap_with(other, "sub", 1)
    moved_near = call(
        lambda *refs: permute_kernel(2 * capacity, *refs),
        "permute_near",
        (key, operators),
        array((3 * capacity, clusters * rows), BF16),
        8,
        3000000000,
    )
    moved_far = call(
        lambda *refs: permute_kernel(0, *refs),
        "permute_far",
        (key, operators),
        array((2 * capacity, clusters * rows), BF16),
        8,
        2000000000,
    )
    early = call(
        lambda *refs: early_kernel(capacity, *refs),
        "stress_early",
        (moved_near, other, own, cross),
        array((clusters, modes, rows), F32),
        8,
        500000000,
    )
    stresses, energy = call(
        lambda *refs: late_kernel(capacity, 0.5 / (modes * mode_count), *refs),
        "stress_late",
        (modal_weight.reshape(modes, 1), compliance, early, moved_far, plus, minus),
        (array((clusters, modes, rows), F32), array((clusters, points), F32)),
        8,
        500000000,
    )
    mask = 1
    while 2 * mask < mode_count:
        energy = energy + swap_with(energy, "mode", mask)
        mask *= 2
    arrived = swap_with(energy, "mode", mask)
    stresses = pl.pallas_call(
        store_kernel,
        out_shape=array((clusters, modes, rows), F32),
        in_specs=[vmem],
        out_specs=hbm,
        scratch_shapes=[pltpu.SemaphoreType.DMA],
        compiler_params=pltpu.CompilerParams(vmem_limit_bytes=4 * 1024 * 1024),
        cost_estimate=pl.CostEstimate(
            flops=500000000, bytes_accessed=2000000, transcendentals=0
        ),
        name="store",
    )(stresses)
    at = lax.axis_index("mode").astype(I32).reshape(1)
    share = clusters * points // mode_count
    strain_energy = call(
        share_kernel,
        "share",
        (at, energy, arrived),
        array((1, share), F32),
        4,
        1000,
        [smem, vmem, vmem],
    )
    return (stresses, strain_energy.reshape(share))


def solution(mesh):
    return jax.shard_map(
        shards,
        mesh=mesh,
        in_specs=(
            P("sub", "mode", None),
            P("sub", None, None),
            P("sub", None, None, None),
            P("mode", "sub"),
            P("mode", "sub"),
            P("mode", "sub"),
            P("sub", None),
            P("sub", None, None),
            P("sub", None),
            P("mode"),
        ),
        out_specs=(P("sub", "mode", None), P(("sub", "mode"))),
        check_vma=False,
    )
```

```python
import jax
import jax.numpy as jnp
from jax import lax
from jax.experimental import pallas as pl
from jax.experimental.pallas import tpu as pltpu
from jax.sharding import PartitionSpec as P


VMEM = pltpu.VMEM
F32 = jnp.float32
BF16 = jnp.bfloat16
I32 = jnp.int32
BASE = 64
GROUP = 4

PLUS, MINUS, PAIR, OWN, CROSS = range(5)


def shift_by(value, axis, by):
    peers = lax.axis_size(axis)
    return lax.ppermute(value, axis, [(i, (i + by) % peers) for i in range(peers)])


def swap_with(value, axis, mask):
    return lax.ppermute(value, axis, [(i, i ^ mask) for i in range(lax.axis_size(axis))])


def swap_across(value, axis):
    peers = lax.axis_size(axis)
    return lax.ppermute(
        value, axis, [(i, (i + 2 * (i % 2) - 1) % peers) for i in range(peers)]
    )


def call(kernel, inputs, outputs, mib, flops, specs=None, scratch=()):
    vmem = pl.BlockSpec(memory_space=VMEM)
    many = isinstance(outputs, tuple)
    nbytes = sum(x.size * x.dtype.itemsize for x in inputs)
    return pl.pallas_call(
        kernel,
        out_shape=outputs,
        in_specs=specs or [vmem] * len(inputs),
        out_specs=(vmem,) * len(outputs) if many else vmem,
        scratch_shapes=list(scratch),
        compiler_params=pltpu.CompilerParams(vmem_limit_bytes=mib * 1024 * 1024),
        cost_estimate=pl.CostEstimate(flops=flops, bytes_accessed=nbytes, transcendentals=0),
    )(*inputs)


def one_hot(target, first, rows):
    local = target - first
    local = jnp.where((local >= 0) & (local < rows), local, -1).astype(F32).astype(BF16)
    ids = lax.broadcasted_iota(I32, (rows, target.shape[1]), 0).astype(F32).astype(BF16)
    hit = ids == jnp.broadcast_to(local, ids.shape)
    return jnp.where(hit, jnp.ones((), BF16), jnp.zeros((), BF16))


def list_rows(key, digits, group, capacity):
    total = None
    for cluster, values in enumerate(digits):
        pick = jnp.concatenate(
            [
                one_hot(key[cluster : cluster + 1, :], group * capacity + at, 128)
                for at in range(0, capacity, 128)
            ],
            axis=0,
        )
        part = lax.dot_general(
            values, pick, (((1,), (1,)), ((), ())), preferred_element_type=F32
        )
        total = part if total is None else total + part
    return [
        total[digit : digit + 1, at : at + 128]
        for digit in (0, 1)
        for at in range(0, capacity, 128)
    ]


def digit_rows(local, clusters):
    high = lax.div(local, jnp.int32(BASE))
    low = local - high * BASE
    return [
        jnp.concatenate([high[c : c + 1, :], low[c : c + 1, :]], axis=0).astype(F32).astype(BF16)
        for c in range(clusters)
    ]


def filled(rows, count):
    lanes = rows[0].shape[1]
    rest = count - sum(row.shape[0] for row in rows)
    return jnp.concatenate(rows + [jnp.zeros((rest, lanes), F32)], axis=0)


def unpacked(block, start, capacity):
    parts = capacity // 128
    block = block.astype(F32)
    high = [block[start + i : start + i + 1, :] for i in range(parts)]
    low = [block[start + parts + i : start + parts + i + 1, :] for i in range(parts)]
    wanted = jnp.concatenate(high, axis=1) * float(BASE) + jnp.concatenate(low, axis=1)
    return wanted.astype(I32)


def list_height(capacity, lists):
    return (2 * capacity // 128 * lists + 15) // 16 * 16


def index_kernel(sub_count, dof_count, capacity, me_ref, rows_ref, key_ref, local_ref, lists_ref):
    clusters, width = rows_ref.shape
    high = (clusters + 7) // 8 * 8
    row = jnp.concatenate(
        [rows_ref[...], jnp.full((high - clusters, width), -1, I32)], axis=0
    )
    before = lax.broadcasted_iota(I32, (width, width), 0)
    after = lax.broadcasted_iota(I32, (width, width), 1)
    upper = jnp.where(before <= after, 1.0, 0.0).astype(BF16)
    me = me_ref[0]
    odd = lax.rem(me, 2)
    source = lax.div(row, jnp.int32(dof_count))
    local = row - source * dof_count
    distance = source - me
    distance = jnp.where(distance < 0, distance + sub_count, distance)
    offset = jnp.where(distance > sub_count // 2, distance - sub_count, distance)
    cross = 2 * odd - 1
    classes = (2, -2, -cross, 0, cross)
    masks = jnp.concatenate(
        [jnp.where((offset == each) & (row >= 0), 1.0, 0.0) for each in classes], axis=0
    )
    counts = jnp.dot(masks.astype(BF16), upper, preferred_element_type=F32)
    key = jnp.zeros((clusters, width), F32)
    for number in range(len(classes)):
        at = number * high
        carried = jnp.full((1, 1), float(number * capacity - 1), F32)
        placed = []
        for cluster in range(clusters):
            count = counts[at + cluster : at + cluster + 1, :]
            placed.append(count + carried)
            carried = carried + count[:, width - 1 : width]
        key = key + masks[at : at + clusters, :] * jnp.concatenate(placed, axis=0)
    key = key.astype(I32)
    local = local[:clusters, :]
    key_ref[...] = key
    local_ref[...] = local
    digits = digit_rows(local, clusters)
    height = list_height(capacity, 1)
    for number, group in enumerate((PLUS, MINUS, CROSS)):
        lists_ref[number * height : (number + 1) * height, :] = filled(
            list_rows(key, digits, group, capacity), height
        )


def pack_kernel(
    capacity,
    rides,
    me_ref,
    one_ref,
    two_ref,
    three_ref,
    lists_ref,
    near_ref,
    diag_ref,
    far_ref,
    one_t_ref,
    *rest,
):
    quarter, eighth = two_ref.shape[0], three_ref.shape[0]
    tall = 2 * capacity // 128
    height = list_height(capacity, 1)
    tail = list_height(capacity, 2)
    plus, minus, relay = [
        lists_ref[number * height : number * height + tall, :] for number in range(3)
    ]
    up = filled([plus, relay], tail)
    down = filled([minus, relay], tail)
    near_ref[:quarter, :] = two_ref[...]
    near_ref[quarter : quarter + eighth, :] = three_ref[...]
    diag_ref[:eighth, :] = three_ref[...]
    far_ref[...] = three_ref[...]
    lanes = near_ref.shape[1]
    if rides:
        low = lax.rem(lax.div(me_ref[0], 2), 2) == 0
        slots = (
            (near_ref, quarter + eighth, jnp.where(low, up, down)),
            (diag_ref, eighth, jnp.where(low, down, up)),
        )
    else:
        slots = ((rest[0], 0, up), (rest[1], 0, down))
    for ref, at, value in slots:
        ref[at : at + tail, :] = jnp.zeros((tail, lanes), BF16)
        ref[at : at + tail, :128] = value.astype(BF16)
    one_t_ref[...] = one_ref[...].astype(F32).T.astype(BF16)


def lists_kernel(capacity, key_ref, local_ref, out_ref):
    clusters = key_ref.shape[0]
    key = key_ref[...]
    digits = digit_rows(local_ref[...], clusters)
    height = list_height(capacity, 1)
    for number, group in enumerate((PAIR, OWN)):
        rows = list_rows(key, digits, group, capacity)
        out_ref[number * height : (number + 1) * height, :] = filled(rows, height)


def relay_kernel(
    capacity,
    rides,
    me_ref,
    one_ref,
    two_ref,
    three_ref,
    near_ref,
    diag_ref,
    far_ref,
    lists_ref,
    *rest,
):
    wants_ref, bag_ref = rest[-1], rest[-2]
    quarter, eighth = two_ref.shape[0], three_ref.shape[0]
    tall = 2 * capacity // 128
    tail = list_height(capacity, 2)
    at = 0
    for value in (
        one_ref[...],
        two_ref[...],
        three_ref[...],
        near_ref[: quarter + eighth, :],
        diag_ref[:eighth, :],
        far_ref[...],
    ):
        bag_ref[at : at + value.shape[0], :] = value
        at += value.shape[0]
    if rides:
        beside = near_ref[quarter + eighth :, :128].astype(F32)
        opposite = diag_ref[eighth:, :128].astype(F32)
        low = lax.rem(lax.div(me_ref[0], 2), 2) == 0
        from_behind = jnp.where(low, opposite, beside)
        from_ahead = jnp.where(low, beside, opposite)
    else:
        from_behind = rest[0][:, :128].astype(F32)
        from_ahead = rest[1][:, :128].astype(F32)
    odd = lax.rem(me_ref[0], 2) == 1
    relayed = jnp.where(odd, from_behind, from_ahead)[tall : 2 * tall, :]
    bag_ref[at : at + tail, :] = jnp.zeros((tail, bag_ref.shape[1]), BF16)
    bag_ref[at : at + tail, :128] = filled([lists_ref[:tall, :], relayed], tail).astype(BF16)
    wants_ref[...] = filled([from_behind[:tall, :], from_ahead[:tall, :]], tail)


def direct_kernel(coords_ref, modes_ref, out_ref):
    leaves = coords_ref.shape[0]
    width = modes_ref.shape[2]
    for leaf in range(leaves):
        out_ref[:, leaf * width : (leaf + 1) * width] = jnp.dot(
            coords_ref[leaf], modes_ref[leaf], preferred_element_type=F32
        )


def gathered(disp_ref, wanted):
    depth = 256
    total = None
    for at in range(0, disp_ref.shape[1], depth):
        part = jnp.dot(
            disp_ref[:, at : at + depth], one_hot(wanted, at, depth), preferred_element_type=F32
        )
        total = part if total is None else total + part
    return total.astype(BF16)


def displace_kernel(
    capacity,
    me_ref,
    direct_ref,
    couple_ref,
    mine_ref,
    pair_ref,
    wants_ref,
    lists_ref,
    disp_ref,
    wanted_ref,
    cross_ref,
    anc_t,
):
    leaves, levels, block, width = couple_ref.shape
    me = me_ref[0]
    odd = lax.rem(me, 2)
    chip = lax.rem(lax.div(me, 2), GROUP)
    near = chip + 1 - 2 * lax.rem(chip, 2)
    far = lax.rem(chip + 2, GROUP)
    diag = lax.rem(near + 2, GROUP)
    half, quarter, eighth = block // 2, block // 4, block // 8

    def put(level, at, rows, value):
        anc_t[pl.ds(pl.multiple_of(level * block + at * rows, rows), rows), :] = value

    for core, ref in ((odd, mine_ref), (1 - odd, pair_ref)):
        pieces = (
            (0, core, half),
            (1, 2 * lax.rem(chip, 2) + core, quarter),
            (2, 2 * chip + core, eighth),
            (1, 2 * lax.rem(near, 2) + core, quarter),
            (2, 2 * near + core, eighth),
            (2, 2 * diag + core, eighth),
            (2, 2 * far + core, eighth),
        )
        start = 0
        for level, at, rows in pieces:
            put(level, at, rows, ref[start : start + rows, :])
            start += rows

    anc = anc_t[...].astype(F32).T.astype(BF16)
    for leaf in range(leaves):
        value = direct_ref[:, leaf * width : (leaf + 1) * width]
        for level in range(levels):
            value = value + jnp.dot(
                anc[:, level * block : (level + 1) * block],
                couple_ref[leaf, level],
                preferred_element_type=F32,
            )
        disp_ref[:, leaf * width : (leaf + 1) * width] = value.astype(BF16)

    tall = 2 * capacity // 128
    height = list_height(capacity, 1)
    tail = list_height(capacity, 2)
    ours = pair_ref[start : start + tail, :128]
    wants = wants_ref[...]
    wanted_ref[:, :capacity] = unpacked(wants, 0, capacity)
    wanted_ref[:, capacity : 2 * capacity] = unpacked(wants, tall, capacity)
    wanted_ref[:, 2 * capacity : 3 * capacity] = unpacked(ours, 0, capacity)
    wanted_ref[:, 3 * capacity :] = unpacked(lists_ref[height : 2 * height, :], 0, capacity)
    cross_ref[...] = gathered(disp_ref, unpacked(ours, tall, capacity))


def gather_kernel(capacity, first, disp_ref, wanted_ref, left_ref, right_ref):
    both = gathered(
        disp_ref, wanted_ref[:, first * capacity : (first + 2) * capacity]
    )
    left_ref[...] = both[:, :capacity]
    right_ref[...] = both[:, capacity:]


def permute_kernel(first, key_ref, operators_ref, out_ref):
    clusters, _, rows = operators_ref.shape
    tile = 384
    for part in range(out_ref.shape[0] // tile):
        for cluster in range(clusters):
            for at in range(0, tile, 128):
                pick = one_hot(
                    key_ref[cluster : cluster + 1, :], first + part * tile + at, 128
                )
                moved = jnp.dot(pick, operators_ref[cluster], preferred_element_type=F32)
                start = part * tile + at
                out_ref[start : start + 128, cluster * rows : (cluster + 1) * rows] = (
                    moved.astype(BF16)
                )


def early_kernel(capacity, moved_ref, pair_ref, own_ref, cross_ref, out_ref):
    clusters, _, rows = out_ref.shape
    for cluster in range(clusters):
        value = None
        for number, ref in enumerate((pair_ref, own_ref, cross_ref)):
            part = jnp.dot(
                ref[...],
                moved_ref[
                    number * capacity : (number + 1) * capacity,
                    cluster * rows : (cluster + 1) * rows,
                ],
                preferred_element_type=F32,
            )
            value = part if value is None else value + part
        out_ref[cluster] = value


def late_kernel(
    capacity,
    scale,
    weight_ref,
    compliance_ref,
    early_ref,
    moved_ref,
    plus_ref,
    minus_ref,
    stress_ref,
    energy_ref,
):
    clusters, modes, rows = stress_ref.shape
    points = energy_ref.shape[1]
    weight = jnp.broadcast_to(weight_ref[...], (8, modes)).T[:, :1]
    for cluster in range(clusters):
        value = early_ref[cluster]
        for number, ref in enumerate((plus_ref, minus_ref)):
            value = value + jnp.dot(
                ref[...],
                moved_ref[
                    number * capacity : (number + 1) * capacity,
                    cluster * rows : (cluster + 1) * rows,
                ],
                preferred_element_type=F32,
            )
        stress_ref[cluster] = value
        square = jnp.sum(value * value * weight, axis=0, keepdims=True)
        square = square * compliance_ref[cluster : cluster + 1, :]
        term = square[:, :points]
        for part in range(1, rows // points):
            term = term + square[:, part * points : (part + 1) * points]
        energy_ref[cluster : cluster + 1, :] = term * scale


def store_kernel(source_ref, target_hbm, sem):
    move = pltpu.make_async_copy(source_ref, target_hbm, sem)
    move.start()
    move.wait()


def share_kernel(at_ref, mine_ref, other_ref, out_ref):
    clusters, points = mine_ref.shape
    total = mine_ref[...] + other_ref[...]
    row = [total[c : c + 1, :] for c in range(clusters)]
    lanes = (clusters * points + 127) // 128 * 128
    if lanes > clusters * points:
        row.append(jnp.zeros((1, lanes - clusters * points), F32))
    flat = jnp.broadcast_to(jnp.concatenate(row, axis=1), (8, lanes))
    share = out_ref.shape[1]
    moved = pltpu.roll(flat, lanes - at_ref[0] * share, 1)
    out_ref[...] = moved[0:1, :share]


def shards(
    leaf_coords,
    leaf_modes,
    constraint_modes,
    sep_one,
    sep_two,
    sep_three,
    cluster_rows,
    operators,
    compliance,
    modal_weight,
):
    sub_count = lax.axis_size("sub")
    mode_count = lax.axis_size("mode")
    me = lax.axis_index("sub").astype(I32).reshape(1)
    leaves, modes, _ = leaf_coords.shape
    width = leaf_modes.shape[2]
    dof_count = leaves * width
    levels, block = constraint_modes.shape[1:3]
    clusters, slots = cluster_rows.shape
    rows = operators.shape[2]
    points = rows // 6
    capacity = clusters * slots // 4
    smem = pl.BlockSpec(memory_space=pltpu.SMEM)
    vmem = pl.BlockSpec(memory_space=VMEM)
    hbm = pl.BlockSpec(memory_space=pltpu.HBM)
    array = jax.ShapeDtypeStruct
    half, quarter, eighth = sep_one.shape[1], sep_two.shape[1], sep_three.shape[1]

    height = list_height(capacity, 1)
    tail = list_height(capacity, 2)
    rides = sub_count == 2 * GROUP
    two_t, three_t = sep_two.T, sep_three.T

    key, local, leaving = call(
        lambda *refs: index_kernel(sub_count, dof_count, capacity, *refs),
        (me, cluster_rows),
        (
            array((clusters, slots), I32),
            array((clusters, slots), I32),
            array((3 * height, 128), F32),
        ),
        8,
        1000000000,
        [smem, vmem],
    )
    extra = tail if rides else 0
    spare = () if rides else (array((tail, modes), BF16),) * 2
    near, diag, far, one_t, *loose = call(
        lambda *refs: pack_kernel(capacity, rides, *refs),
        (me, sep_one, two_t, three_t, leaving),
        (
            array((quarter + eighth + extra, modes), BF16),
            array((eighth + extra, modes), BF16),
            array((eighth, modes), BF16),
            array((half, modes), BF16),
        )
        + spare,
        4,
        10000000,
        [smem, vmem, vmem, vmem, vmem],
    )
    diag = swap_with(diag, "sub", 6)
    near = swap_with(near, "sub", 2)
    far = swap_with(far, "sub", 4)
    if loose:
        loose = [shift_by(loose[0], "sub", 2), shift_by(loose[1], "sub", -2)]
    lists = call(
        lambda *refs: lists_kernel(capacity, *refs),
        (key, local),
        array((2 * height, 128), F32),
        8,
        1000000000,
    )
    direct = call(
        direct_kernel,
        (leaf_coords, leaf_modes),
        array((modes, dof_count), F32),
        4,
        1500000000,
    )
    moved_near = call(
        lambda *refs: permute_kernel(2 * capacity, *refs),
        (key, operators),
        array((3 * capacity, clusters * rows), BF16),
        8,
        3000000000,
    )
    held = half + 2 * quarter + 4 * eighth + tail
    bag, wants = call(
        lambda *refs: relay_kernel(capacity, rides, *refs),
        (me, one_t, two_t, three_t, near, diag, far, lists, *loose),
        (array((held, modes), BF16), array((tail, 128), F32)),
        4,
        10000000,
        [smem] + [vmem] * (7 + len(loose)),
    )
    pair = swap_with(bag, "sub", 1)
    disp, wanted, cross = call(
        lambda *refs: displace_kernel(capacity, *refs),
        (me, direct, constraint_modes, bag, pair, wants, lists),
        (
            array((modes, dof_count), BF16),
            array((1, 4 * capacity), I32),
            array((modes, capacity), BF16),
        ),
        12,
        3000000000,
        [smem] + [vmem] * 6,
        [VMEM((levels * block, modes), BF16)],
    )
    cross = swap_across(cross, "sub")
    flow = array((modes, capacity), BF16)
    plus, minus = call(
        lambda *refs: gather_kernel(capacity, 0, *refs),
        (disp, wanted),
        (flow, flow),
        12,
        2000000000,
    )
    plus = shift_by(plus, "sub", -2)
    minus = shift_by(minus, "sub", 2)
    other, own = call(
        lambda *refs: gather_kernel(capacity, 2, *refs),
        (disp, wanted),
        (flow, flow),
        12,
        2000000000,
    )
    other = swap_with(other, "sub", 1)
    moved_far = call(
        lambda *refs: permute_kernel(0, *refs),
        (key, operators),
        array((2 * capacity, clusters * rows), BF16),
        8,
        2000000000,
    )
    early = call(
        lambda *refs: early_kernel(capacity, *refs),
        (moved_near, other, own, cross),
        array((clusters, modes, rows), F32),
        8,
        500000000,
    )
    stresses, energy = call(
        lambda *refs: late_kernel(capacity, 0.5 / (modes * mode_count), *refs),
        (modal_weight.reshape(1, modes), compliance, early, moved_far, plus, minus),
        (array((clusters, modes, rows), F32), array((clusters, points), F32)),
        8,
        500000000,
    )
    mask = 1
    while 2 * mask < mode_count:
        energy = energy + swap_with(energy, "mode", mask)
        mask *= 2
    arrived = swap_with(energy, "mode", mask)
    stresses = pl.pallas_call(
        store_kernel,
        out_shape=array((clusters, modes, rows), F32),
        in_specs=[vmem],
        out_specs=hbm,
        scratch_shapes=[pltpu.SemaphoreType.DMA],
        compiler_params=pltpu.CompilerParams(vmem_limit_bytes=4 * 1024 * 1024),
        cost_estimate=pl.CostEstimate(
            flops=500000000, bytes_accessed=2000000, transcendentals=0
        ),
        name="store",
    )(stresses)
    at = lax.axis_index("mode").astype(I32).reshape(1)
    share = clusters * points // mode_count
    strain_energy = call(
        share_kernel,
        (at, energy, arrived),
        array((1, share), F32),
        4,
        1000,
        [smem, vmem, vmem],
    )
    return (stresses, strain_energy.reshape(share))


def solution(mesh):
    return jax.shard_map(
        shards,
        mesh=mesh,
        in_specs=(
            P("sub", "mode", None),
            P("sub", None, None),
            P("sub", None, None, None),
            P("mode", "sub"),
            P("mode", "sub"),
            P("mode", "sub"),
            P("sub", None),
            P("sub", None, None),
            P("sub", None),
            P("mode"),
        ),
        out_specs=(P("sub", "mode", None), P(("sub", "mode"))),
        check_vma=False,
    )
```

```python
import jax
import jax.numpy as jnp
from jax import lax
from jax.experimental import pallas as pl
from jax.experimental.pallas import tpu as pltpu
from jax.sharding import PartitionSpec as P


VMEM = pltpu.VMEM
F32 = jnp.float32
BF16 = jnp.bfloat16
I32 = jnp.int32
BASE = 64
GROUP = 4

PLUS, MINUS, PAIR, OWN, CROSS = range(5)


def shift_by(value, axis, by):
    peers = lax.axis_size(axis)
    return lax.ppermute(value, axis, [(i, (i + by) % peers) for i in range(peers)])


def swap_with(value, axis, mask):
    return lax.ppermute(value, axis, [(i, i ^ mask) for i in range(lax.axis_size(axis))])


def swap_across(value, axis):
    peers = lax.axis_size(axis)
    return lax.ppermute(
        value, axis, [(i, (i + 2 * (i % 2) - 1) % peers) for i in range(peers)]
    )


def call(kernel, inputs, outputs, mib, flops, specs=None, scratch=()):
    vmem = pl.BlockSpec(memory_space=VMEM)
    many = isinstance(outputs, tuple)
    nbytes = sum(x.size * x.dtype.itemsize for x in inputs)
    return pl.pallas_call(
        kernel,
        out_shape=outputs,
        in_specs=specs or [vmem] * len(inputs),
        out_specs=(vmem,) * len(outputs) if many else vmem,
        scratch_shapes=list(scratch),
        compiler_params=pltpu.CompilerParams(vmem_limit_bytes=mib * 1024 * 1024),
        cost_estimate=pl.CostEstimate(flops=flops, bytes_accessed=nbytes, transcendentals=0),
    )(*inputs)


def one_hot(target, first, rows):
    local = target - first
    local = jnp.where((local >= 0) & (local < rows), local, -1).astype(F32).astype(BF16)
    ids = lax.broadcasted_iota(I32, (rows, target.shape[1]), 0).astype(F32).astype(BF16)
    hit = ids == jnp.broadcast_to(local, ids.shape)
    return jnp.where(hit, jnp.ones((), BF16), jnp.zeros((), BF16))


def list_rows(lists, group, capacity):
    parts = capacity // 128
    low = lists.shape[0] // 2 + group * parts
    return [lists[group * parts : (group + 1) * parts, :], lists[low : low + parts, :]]


def filled(rows, count):
    lanes = rows[0].shape[1]
    rest = count - sum(row.shape[0] for row in rows)
    return jnp.concatenate(rows + [jnp.zeros((rest, lanes), F32)], axis=0)


def unpacked(block, start, capacity):
    parts = capacity // 128
    block = block.astype(F32)
    high = [block[start + i : start + i + 1, :] for i in range(parts)]
    low = [block[start + parts + i : start + parts + i + 1, :] for i in range(parts)]
    wanted = jnp.concatenate(high, axis=1) * float(BASE) + jnp.concatenate(low, axis=1)
    return wanted.astype(I32)


def list_height(capacity, lists):
    return (2 * capacity // 128 * lists + 15) // 16 * 16


def index_kernel(sub_count, dof_count, capacity, me_ref, rows_ref, key_ref, lists_ref):
    clusters, width = rows_ref.shape
    high = (clusters + 7) // 8 * 8
    row = jnp.concatenate(
        [rows_ref[...], jnp.full((high - clusters, width), -1, I32)], axis=0
    )
    before = lax.broadcasted_iota(I32, (width, width), 0)
    after = lax.broadcasted_iota(I32, (width, width), 1)
    upper = jnp.where(before <= after, 1.0, 0.0).astype(BF16)
    me = me_ref[0]
    odd = lax.rem(me, 2)
    source = lax.div(row, jnp.int32(dof_count))
    local = row - source * dof_count
    distance = source - me
    distance = jnp.where(distance < 0, distance + sub_count, distance)
    offset = jnp.where(distance > sub_count // 2, distance - sub_count, distance)
    cross = 2 * odd - 1
    classes = (2, -2, -cross, 0, cross)
    masks = jnp.concatenate(
        [jnp.where((offset == each) & (row >= 0), 1.0, 0.0) for each in classes], axis=0
    )
    counts = jnp.dot(masks.astype(BF16), upper, preferred_element_type=F32)
    key = jnp.zeros((clusters, width), F32)
    for number in range(len(classes)):
        at = number * high
        carried = jnp.full((1, 1), float(number * capacity - 1), F32)
        placed = []
        for cluster in range(clusters):
            count = counts[at + cluster : at + cluster + 1, :]
            placed.append(count + carried)
            carried = carried + count[:, width - 1 : width]
        key = key + masks[at : at + clusters, :] * jnp.concatenate(placed, axis=0)
    key = key.astype(I32)
    key_ref[...] = key
    tall = lists_ref.shape[0] // 2
    rank_high = lax.div(key, jnp.int32(128))
    rank_low = key - rank_high * 128
    digit_high = lax.div(local, jnp.int32(BASE))
    digits = (digit_high.astype(F32), (local - digit_high * BASE).astype(F32))
    ids = lax.broadcasted_iota(I32, (tall, width), 0)
    values, picks = [], []
    for cluster in range(clusters):
        at = slice(cluster, cluster + 1)
        hit = ids == rank_high[at, :]
        values.append(
            jnp.concatenate([jnp.where(hit, digit[at, :], 0.0) for digit in digits], axis=0)
        )
        picks.append(one_hot(rank_low[at, :], 0, 128))
    lists_ref[...] = lax.dot_general(
        jnp.concatenate(values, axis=1).astype(BF16),
        jnp.concatenate(picks, axis=1),
        (((1,), (1,)), ((), ())),
        preferred_element_type=F32,
    )


def pack_kernel(
    capacity,
    rides,
    me_ref,
    one_ref,
    two_ref,
    three_ref,
    lists_ref,
    near_ref,
    diag_ref,
    far_ref,
    one_t_ref,
    *rest,
):
    quarter, eighth = two_ref.shape[0], three_ref.shape[0]
    tail = list_height(capacity, 2)
    lists = lists_ref[...]
    relay = list_rows(lists, CROSS, capacity)
    up = filled(list_rows(lists, PLUS, capacity) + relay, tail)
    down = filled(list_rows(lists, MINUS, capacity) + relay, tail)
    near_ref[:quarter, :] = two_ref[...]
    near_ref[quarter : quarter + eighth, :] = three_ref[...]
    diag_ref[:eighth, :] = three_ref[...]
    far_ref[...] = three_ref[...]
    lanes = near_ref.shape[1]
    if rides:
        low = lax.rem(lax.div(me_ref[0], 2), 2) == 0
        slots = (
            (near_ref, quarter + eighth, jnp.where(low, up, down)),
            (diag_ref, eighth, jnp.where(low, down, up)),
        )
    else:
        slots = ((rest[0], 0, up), (rest[1], 0, down))
    for ref, at, value in slots:
        ref[at : at + tail, :] = jnp.zeros((tail, lanes), BF16)
        ref[at : at + tail, :128] = value.astype(BF16)
    one_t_ref[...] = one_ref[...].astype(F32).T.astype(BF16)


def relay_kernel(
    capacity,
    rides,
    me_ref,
    one_ref,
    two_ref,
    three_ref,
    near_ref,
    diag_ref,
    far_ref,
    lists_ref,
    *rest,
):
    wants_ref, bag_ref = rest[-1], rest[-2]
    quarter, eighth = two_ref.shape[0], three_ref.shape[0]
    tall = 2 * capacity // 128
    tail = list_height(capacity, 2)
    at = 0
    for value in (
        one_ref[...],
        two_ref[...],
        three_ref[...],
        near_ref[: quarter + eighth, :],
        diag_ref[:eighth, :],
        far_ref[...],
    ):
        bag_ref[at : at + value.shape[0], :] = value
        at += value.shape[0]
    if rides:
        beside = near_ref[quarter + eighth :, :128].astype(F32)
        opposite = diag_ref[eighth:, :128].astype(F32)
        low = lax.rem(lax.div(me_ref[0], 2), 2) == 0
        from_behind = jnp.where(low, opposite, beside)
        from_ahead = jnp.where(low, beside, opposite)
    else:
        from_behind = rest[0][:, :128].astype(F32)
        from_ahead = rest[1][:, :128].astype(F32)
    odd = lax.rem(me_ref[0], 2) == 1
    relayed = jnp.where(odd, from_behind, from_ahead)[tall : 2 * tall, :]
    bag_ref[at : at + tail, :] = jnp.zeros((tail, bag_ref.shape[1]), BF16)
    bag_ref[at : at + tail, :128] = filled(
        list_rows(lists_ref[...], PAIR, capacity) + [relayed], tail
    ).astype(BF16)
    wants_ref[...] = filled([from_behind[:tall, :], from_ahead[:tall, :]], tail)


def direct_kernel(coords_ref, modes_ref, out_ref):
    leaves = coords_ref.shape[0]
    width = modes_ref.shape[2]
    for leaf in range(leaves):
        out_ref[:, leaf * width : (leaf + 1) * width] = jnp.dot(
            coords_ref[leaf], modes_ref[leaf], preferred_element_type=F32
        )


def gathered(disp_ref, wanted):
    depth = 256
    total = None
    for at in range(0, disp_ref.shape[1], depth):
        part = jnp.dot(
            disp_ref[:, at : at + depth], one_hot(wanted, at, depth), preferred_element_type=F32
        )
        total = part if total is None else total + part
    return total.astype(BF16)


def coupled(me, core, couple_ref, bag_ref):
    leaves, _, block, width = couple_ref.shape
    chip = lax.rem(lax.div(me, 2), GROUP)
    near = chip + 1 - 2 * lax.rem(chip, 2)
    far = lax.rem(chip + 2, GROUP)
    diag = lax.rem(near + 2, GROUP)
    half, quarter, eighth = block // 2, block // 4, block // 8
    pieces = (
        (0, core, half),
        (1, 2 * lax.rem(chip, 2) + core, quarter),
        (2, 2 * chip + core, eighth),
        (1, 2 * lax.rem(near, 2) + core, quarter),
        (2, 2 * near + core, eighth),
        (2, 2 * diag + core, eighth),
        (2, 2 * far + core, eighth),
    )
    held = sum(rows for level, at, rows in pieces)
    anc = bag_ref[:held, :].astype(F32).T.astype(BF16)
    for leaf in range(leaves):
        weights = jnp.concatenate(
            [
                couple_ref[leaf, level, pl.ds(pl.multiple_of(at * rows, rows), rows), :]
                for level, at, rows in pieces
            ],
            axis=0,
        )
        columns = slice(leaf * width, (leaf + 1) * width)
        yield columns, jnp.dot(anc, weights, preferred_element_type=F32)


def partial_kernel(me_ref, direct_ref, couple_ref, bag_ref, out_ref):
    me = me_ref[0]
    for columns, value in coupled(me, lax.rem(me, 2), couple_ref, bag_ref):
        out_ref[:, columns] = direct_ref[:, columns] + value


def displace_kernel(
    capacity,
    me_ref,
    partial_ref,
    couple_ref,
    pair_ref,
    wants_ref,
    lists_ref,
    disp_ref,
    wanted_ref,
    cross_ref,
):
    me = me_ref[0]
    for columns, value in coupled(me, 1 - lax.rem(me, 2), couple_ref, pair_ref):
        disp_ref[:, columns] = (partial_ref[:, columns] + value).astype(BF16)
    tall = 2 * capacity // 128
    tail = list_height(capacity, 2)
    ours = pair_ref[pair_ref.shape[0] - tail :, :128]
    wants = wants_ref[...]
    wanted_ref[:, :capacity] = unpacked(wants, 0, capacity)
    wanted_ref[:, capacity : 2 * capacity] = unpacked(wants, tall, capacity)
    wanted_ref[:, 2 * capacity : 3 * capacity] = unpacked(ours, 0, capacity)
    wanted_ref[:, 3 * capacity :] = unpacked(
        filled(list_rows(lists_ref[...], OWN, capacity), tail), 0, capacity
    )
    cross_ref[...] = gathered(disp_ref, unpacked(ours, tall, capacity))


def gather_kernel(capacity, first, disp_ref, wanted_ref, left_ref, right_ref):
    both = gathered(
        disp_ref, wanted_ref[:, first * capacity : (first + 2) * capacity]
    )
    left_ref[...] = both[:, :capacity]
    right_ref[...] = both[:, capacity:]


def permute_kernel(first, key_ref, operators_ref, out_ref):
    clusters, _, rows = operators_ref.shape
    tile = 384
    for part in range(out_ref.shape[0] // tile):
        for cluster in range(clusters):
            for at in range(0, tile, 128):
                pick = one_hot(
                    key_ref[cluster : cluster + 1, :], first + part * tile + at, 128
                )
                moved = jnp.dot(pick, operators_ref[cluster], preferred_element_type=F32)
                start = part * tile + at
                out_ref[start : start + 128, cluster * rows : (cluster + 1) * rows] = (
                    moved.astype(BF16)
                )


def early_kernel(capacity, moved_ref, pair_ref, own_ref, cross_ref, out_ref):
    clusters, _, rows = out_ref.shape
    for cluster in range(clusters):
        value = None
        for number, ref in enumerate((pair_ref, own_ref, cross_ref)):
            part = jnp.dot(
                ref[...],
                moved_ref[
                    number * capacity : (number + 1) * capacity,
                    cluster * rows : (cluster + 1) * rows,
                ],
                preferred_element_type=F32,
            )
            value = part if value is None else value + part
        out_ref[cluster] = value


def late_kernel(
    scale,
    weight_ref,
    compliance_ref,
    early_ref,
    moved_ref,
    plus_ref,
    minus_ref,
    stress_ref,
    energy_ref,
):
    clusters, modes, rows = stress_ref.shape
    points = energy_ref.shape[1]
    weight = jnp.broadcast_to(weight_ref[...], (8, modes)).T[:, :1]
    arrived = jnp.concatenate([plus_ref[...], minus_ref[...]], axis=1)
    late = jnp.dot(arrived, moved_ref[...], preferred_element_type=F32)
    for cluster in range(clusters):
        value = early_ref[cluster] + late[:, cluster * rows : (cluster + 1) * rows]
        stress_ref[cluster] = value
        square = jnp.sum(value * value * weight, axis=0, keepdims=True)
        square = square * compliance_ref[cluster : cluster + 1, :]
        term = square[:, :points]
        for part in range(1, rows // points):
            term = term + square[:, part * points : (part + 1) * points]
        energy_ref[cluster : cluster + 1, :] = term * scale


def store_kernel(source_ref, target_hbm, sem):
    move = pltpu.make_async_copy(source_ref, target_hbm, sem)
    move.start()
    move.wait()


def share_kernel(at_ref, mine_ref, other_ref, out_ref):
    clusters, points = mine_ref.shape
    total = mine_ref[...] + other_ref[...]
    row = [total[c : c + 1, :] for c in range(clusters)]
    lanes = (clusters * points + 127) // 128 * 128
    if lanes > clusters * points:
        row.append(jnp.zeros((1, lanes - clusters * points), F32))
    flat = jnp.broadcast_to(jnp.concatenate(row, axis=1), (8, lanes))
    share = out_ref.shape[1]
    moved = pltpu.roll(flat, lanes - at_ref[0] * share, 1)
    out_ref[...] = moved[0:1, :share]


def shards(
    leaf_coords,
    leaf_modes,
    constraint_modes,
    sep_one,
    sep_two,
    sep_three,
    cluster_rows,
    operators,
    compliance,
    modal_weight,
):
    sub_count = lax.axis_size("sub")
    mode_count = lax.axis_size("mode")
    me = lax.axis_index("sub").astype(I32).reshape(1)
    leaves, modes, _ = leaf_coords.shape
    width = leaf_modes.shape[2]
    dof_count = leaves * width
    clusters, slots = cluster_rows.shape
    rows = operators.shape[2]
    points = rows // 6
    capacity = clusters * slots // 4
    smem = pl.BlockSpec(memory_space=pltpu.SMEM)
    vmem = pl.BlockSpec(memory_space=VMEM)
    hbm = pl.BlockSpec(memory_space=pltpu.HBM)
    array = jax.ShapeDtypeStruct
    half, quarter, eighth = sep_one.shape[1], sep_two.shape[1], sep_three.shape[1]

    tail = list_height(capacity, 2)
    rides = sub_count == 2 * GROUP
    two_t, three_t = sep_two.T, sep_three.T

    tall = (5 * capacity // 128 + 7) // 8 * 8
    key, lists = call(
        lambda *refs: index_kernel(sub_count, dof_count, capacity, *refs),
        (me, cluster_rows),
        (array((clusters, slots), I32), array((2 * tall, 128), F32)),
        8,
        1000000000,
        [smem, vmem],
    )
    extra = tail if rides else 0
    spare = () if rides else (array((tail, modes), BF16),) * 2
    near, diag, far, one_t, *loose = call(
        lambda *refs: pack_kernel(capacity, rides, *refs),
        (me, sep_one, two_t, three_t, lists),
        (
            array((quarter + eighth + extra, modes), BF16),
            array((eighth + extra, modes), BF16),
            array((eighth, modes), BF16),
            array((half, modes), BF16),
        )
        + spare,
        4,
        10000000,
        [smem, vmem, vmem, vmem, vmem],
    )
    diag = swap_with(diag, "sub", 6)
    near = swap_with(near, "sub", 2)
    far = swap_with(far, "sub", 4)
    if loose:
        loose = [shift_by(loose[0], "sub", 2), shift_by(loose[1], "sub", -2)]
    direct = call(
        direct_kernel,
        (leaf_coords, leaf_modes),
        array((modes, dof_count), F32),
        4,
        1500000000,
    )
    moved_near = call(
        lambda *refs: permute_kernel(2 * capacity, *refs),
        (key, operators),
        array((3 * capacity, clusters * rows), BF16),
        8,
        3000000000,
    )
    held = half + 2 * quarter + 4 * eighth + tail
    bag, wants = call(
        lambda *refs: relay_kernel(capacity, rides, *refs),
        (me, one_t, two_t, three_t, near, diag, far, lists, *loose),
        (array((held, modes), BF16), array((tail, 128), F32)),
        4,
        10000000,
        [smem] + [vmem] * (7 + len(loose)),
    )
    pair = swap_with(bag, "sub", 1)
    partial = call(
        partial_kernel,
        (me, direct, constraint_modes, bag),
        array((modes, dof_count), F32),
        8,
        1000000000,
        [smem] + [vmem] * 3,
    )
    disp, wanted, cross = call(
        lambda *refs: displace_kernel(capacity, *refs),
        (me, partial, constraint_modes, pair, wants, lists),
        (
            array((modes, dof_count), BF16),
            array((1, 4 * capacity), I32),
            array((modes, capacity), BF16),
        ),
        12,
        3000000000,
        [smem] + [vmem] * 5,
    )
    cross = swap_across(cross, "sub")
    flow = array((modes, capacity), BF16)
    plus, minus = call(
        lambda *refs: gather_kernel(capacity, 0, *refs),
        (disp, wanted),
        (flow, flow),
        12,
        2000000000,
    )
    plus = shift_by(plus, "sub", -2)
    minus = shift_by(minus, "sub", 2)
    other, own = call(
        lambda *refs: gather_kernel(capacity, 2, *refs),
        (disp, wanted),
        (flow, flow),
        12,
        2000000000,
    )
    other = swap_with(other, "sub", 1)
    moved_far = call(
        lambda *refs: permute_kernel(0, *refs),
        (key, operators),
        array((2 * capacity, clusters * rows), BF16),
        8,
        2000000000,
    )
    early = call(
        lambda *refs: early_kernel(capacity, *refs),
        (moved_near, other, own, cross),
        array((clusters, modes, rows), F32),
        8,
        500000000,
    )
    stresses, energy = call(
        lambda *refs: late_kernel(0.5 / (modes * mode_count), *refs),
        (modal_weight.reshape(1, modes), compliance, early, moved_far, plus, minus),
        (array((clusters, modes, rows), F32), array((clusters, points), F32)),
        8,
        500000000,
    )
    mask = 1
    while 2 * mask < mode_count:
        energy = energy + swap_with(energy, "mode", mask)
        mask *= 2
    arrived = swap_with(energy, "mode", mask)
    stresses = pl.pallas_call(
        store_kernel,
        out_shape=array((clusters, modes, rows), F32),
        in_specs=[vmem],
        out_specs=hbm,
        scratch_shapes=[pltpu.SemaphoreType.DMA],
        compiler_params=pltpu.CompilerParams(vmem_limit_bytes=4 * 1024 * 1024),
        cost_estimate=pl.CostEstimate(
            flops=500000000, bytes_accessed=2000000, transcendentals=0
        ),
        name="store",
    )(stresses)
    at = lax.axis_index("mode").astype(I32).reshape(1)
    share = clusters * points // mode_count
    strain_energy = call(
        share_kernel,
        (at, energy, arrived),
        array((1, share), F32),
        4,
        1000,
        [smem, vmem, vmem],
    )
    return (stresses, strain_energy.reshape(share))


def solution(mesh):
    return jax.shard_map(
        shards,
        mesh=mesh,
        in_specs=(
            P("sub", "mode", None),
            P("sub", None, None),
            P("sub", None, None, None),
            P("mode", "sub"),
            P("mode", "sub"),
            P("mode", "sub"),
            P("sub", None),
            P("sub", None, None),
            P("sub", None),
            P("mode"),
        ),
        out_specs=(P("sub", "mode", None), P(("sub", "mode"))),
        check_vma=False,
    )
```

```python
import jax
import jax.numpy as jnp
from jax import lax
from jax.experimental import pallas as pl
from jax.experimental.pallas import tpu as pltpu
from jax.sharding import PartitionSpec as P


VMEM = pltpu.VMEM
F32 = jnp.float32
BF16 = jnp.bfloat16
I32 = jnp.int32
BASE = 64
GROUP = 4

PLUS, MINUS, PAIR, OWN, CROSS = range(5)


def shift_by(value, axis, by):
    peers = lax.axis_size(axis)
    return lax.ppermute(value, axis, [(i, (i + by) % peers) for i in range(peers)])


def swap_with(value, axis, mask):
    return lax.ppermute(value, axis, [(i, i ^ mask) for i in range(lax.axis_size(axis))])


def swap_across(value, axis):
    peers = lax.axis_size(axis)
    return lax.ppermute(
        value, axis, [(i, (i + 2 * (i % 2) - 1) % peers) for i in range(peers)]
    )


def call(kernel, inputs, outputs, mib, flops, specs=None, scratch=()):
    vmem = pl.BlockSpec(memory_space=VMEM)
    many = isinstance(outputs, tuple)
    nbytes = sum(x.size * x.dtype.itemsize for x in inputs)
    return pl.pallas_call(
        kernel,
        out_shape=outputs,
        in_specs=specs or [vmem] * len(inputs),
        out_specs=(vmem,) * len(outputs) if many else vmem,
        scratch_shapes=list(scratch),
        compiler_params=pltpu.CompilerParams(vmem_limit_bytes=mib * 1024 * 1024),
        cost_estimate=pl.CostEstimate(flops=flops, bytes_accessed=nbytes, transcendentals=0),
    )(*inputs)


def one_hot(target, first, rows):
    local = target - first
    local = jnp.where((local >= 0) & (local < rows), local, -1).astype(F32).astype(BF16)
    ids = lax.broadcasted_iota(I32, (rows, target.shape[1]), 0).astype(F32).astype(BF16)
    hit = ids == jnp.broadcast_to(local, ids.shape)
    return jnp.where(hit, jnp.ones((), BF16), jnp.zeros((), BF16))


def list_rows(lists, group, capacity):
    parts = capacity // 128
    low = lists.shape[0] // 2 + group * parts
    return [lists[group * parts : (group + 1) * parts, :], lists[low : low + parts, :]]


def filled(rows, count):
    lanes = rows[0].shape[1]
    rest = count - sum(row.shape[0] for row in rows)
    if not rest:
        return jnp.concatenate(rows, axis=0)
    return jnp.concatenate(rows + [jnp.zeros((rest, lanes), F32)], axis=0)


def unpacked(block, start, capacity):
    parts = capacity // 128
    block = block.astype(F32)
    high = [block[start + i : start + i + 1, :] for i in range(parts)]
    low = [block[start + parts + i : start + parts + i + 1, :] for i in range(parts)]
    wanted = jnp.concatenate(high, axis=1) * float(BASE) + jnp.concatenate(low, axis=1)
    return wanted.astype(I32)


def list_height(capacity, lists):
    return (2 * capacity // 128 * lists + 15) // 16 * 16


def index_kernel(sub_count, dof_count, capacity, me_ref, rows_ref, key_ref, lists_ref):
    clusters, width = rows_ref.shape
    high = (clusters + 7) // 8 * 8
    row = jnp.concatenate(
        [rows_ref[...], jnp.full((high - clusters, width), -1, I32)], axis=0
    )
    before = lax.broadcasted_iota(I32, (width, width), 0)
    after = lax.broadcasted_iota(I32, (width, width), 1)
    upper = jnp.where(before <= after, 1.0, 0.0).astype(BF16)
    me = me_ref[0]
    odd = lax.rem(me, 2)
    source = lax.div(row, jnp.int32(dof_count))
    local = row - source * dof_count
    distance = source - me
    distance = jnp.where(distance < 0, distance + sub_count, distance)
    offset = jnp.where(distance > sub_count // 2, distance - sub_count, distance)
    cross = 2 * odd - 1
    classes = (2, -2, -cross, 0, cross)
    masks = jnp.concatenate(
        [jnp.where((offset == each) & (row >= 0), 1.0, 0.0) for each in classes], axis=0
    )
    counts = jnp.dot(masks.astype(BF16), upper, preferred_element_type=F32)
    key = jnp.zeros((clusters, width), F32)
    for number in range(len(classes)):
        at = number * high
        carried = jnp.full((1, 1), float(number * capacity - 1), F32)
        placed = []
        for cluster in range(clusters):
            count = counts[at + cluster : at + cluster + 1, :]
            placed.append(count + carried)
            carried = carried + count[:, width - 1 : width]
        key = key + masks[at : at + clusters, :] * jnp.concatenate(placed, axis=0)
    key = key.astype(I32)
    key_ref[...] = key
    tall = lists_ref.shape[0] // 2
    rank_high = lax.div(key, jnp.int32(128))
    rank_low = key - rank_high * 128
    digit_high = lax.div(local, jnp.int32(BASE))
    digits = (digit_high.astype(F32), (local - digit_high * BASE).astype(F32))
    ids = lax.broadcasted_iota(I32, (tall, width), 0)
    values, picks = [], []
    for cluster in range(clusters):
        at = slice(cluster, cluster + 1)
        hit = ids == rank_high[at, :]
        values.append(
            jnp.concatenate([jnp.where(hit, digit[at, :], 0.0) for digit in digits], axis=0)
        )
        picks.append(one_hot(rank_low[at, :], 0, 128))
    lists_ref[...] = lax.dot_general(
        jnp.concatenate(values, axis=1).astype(BF16),
        jnp.concatenate(picks, axis=1),
        (((1,), (1,)), ((), ())),
        preferred_element_type=F32,
    )


def pack_kernel(capacity, one_ref, two_ref, three_ref, lists_ref, bag_ref):
    tail = list_height(capacity, 2)
    lists = lists_ref[...]
    at = 0
    for value in (one_ref[...].astype(F32).T.astype(BF16), two_ref[...], three_ref[...]):
        bag_ref[at : at + value.shape[0], :] = value
        at += value.shape[0]
    put_lists(
        bag_ref, at, list_rows(lists, PAIR, capacity) + list_rows(lists, CROSS, capacity), tail
    )


def put_lists(ref, at, rows, tail):
    ref[at : at + tail, :] = jnp.zeros((tail, ref.shape[1]), BF16)
    ref[at : at + tail, :128] = filled(rows, tail).astype(BF16)


def relay_kernel(
    capacity, rides, half, me_ref, bag_ref, pair_ref, lists_ref, near_ref, diag_ref, far_ref, *rest
):
    tail = list_height(capacity, 2)
    tall = 2 * capacity // 128
    quarter, eighth = half // 2, half // 4
    odd = lax.rem(me_ref[0], 2)
    lists = lists_ref[...]
    relayed = pair_ref[half + quarter + eighth :, :128].astype(F32)[tall : 2 * tall, :]
    up = list_rows(lists, PLUS, capacity) + [relayed]
    down = list_rows(lists, MINUS, capacity) + [relayed]

    def put(ref, at, rows, core, value):
        ref[pl.ds(pl.multiple_of(at + core * rows, rows), rows), :] = value

    for core, ref in ((odd, bag_ref), (1 - odd, pair_ref)):
        two = ref[half : half + quarter, :]
        three = ref[half + quarter : half + quarter + eighth, :]
        put(near_ref, 0, quarter, core, two)
        put(near_ref, 2 * quarter, eighth, core, three)
        put(diag_ref, 0, eighth, core, three)
        put(far_ref, 0, eighth, core, three)
    if rides:
        low = lax.rem(lax.div(me_ref[0], 2), 2) == 0
        up, down = filled(up, tail), filled(down, tail)
        put_lists(near_ref, 2 * (quarter + eighth), [jnp.where(low, up, down)], tail)
        put_lists(diag_ref, 2 * eighth, [jnp.where(low, down, up)], tail)
    else:
        put_lists(rest[0], 0, up, tail)
        put_lists(rest[1], 0, down, tail)


def direct_kernel(coords_ref, modes_ref, out_ref):
    leaves = coords_ref.shape[0]
    width = modes_ref.shape[2]
    for leaf in range(leaves):
        out_ref[:, leaf * width : (leaf + 1) * width] = jnp.dot(
            coords_ref[leaf], modes_ref[leaf], preferred_element_type=F32
        )


def gathered(disp_ref, wanted):
    depth = 256
    total = None
    for at in range(0, disp_ref.shape[1], depth):
        part = jnp.dot(
            disp_ref[:, at : at + depth], one_hot(wanted, at, depth), preferred_element_type=F32
        )
        total = part if total is None else total + part
    return total.astype(BF16)


def coupled(pieces, couple_ref):
    leaves, _, _, width = couple_ref.shape
    anc = jnp.concatenate([value for level, at, value in pieces], axis=0)
    anc = anc.astype(F32).T.astype(BF16)
    for leaf in range(leaves):
        weights = []
        for level, at, value in pieces:
            rows = value.shape[0]
            start = pl.multiple_of(at * rows, rows)
            weights.append(couple_ref[leaf, level, pl.ds(start, rows), :])
        columns = slice(leaf * width, (leaf + 1) * width)
        yield columns, jnp.dot(
            anc, jnp.concatenate(weights, axis=0), preferred_element_type=F32
        )


def places(me):
    chip = lax.rem(lax.div(me, 2), GROUP)
    near = chip + 1 - 2 * lax.rem(chip, 2)
    return chip, near, lax.rem(near + 2, GROUP), lax.rem(chip + 2, GROUP)


def partial_kernel(me_ref, direct_ref, couple_ref, bag_ref, pair_ref, out_ref):
    me = me_ref[0]
    odd = lax.rem(me, 2)
    chip, _, _, _ = places(me)
    block = couple_ref.shape[2]
    half, quarter, eighth = block // 2, block // 4, block // 8
    pieces = []
    for core, ref in ((odd, bag_ref), (1 - odd, pair_ref)):
        pieces += [
            (0, core, ref[:half, :]),
            (1, 2 * lax.rem(chip, 2) + core, ref[half : half + quarter, :]),
            (2, 2 * chip + core, ref[half + quarter : half + quarter + eighth, :]),
        ]
    for columns, value in coupled(pieces, couple_ref):
        out_ref[:, columns] = direct_ref[:, columns] + value


def displace_kernel(
    capacity,
    rides,
    me_ref,
    partial_ref,
    couple_ref,
    pair_ref,
    near_ref,
    diag_ref,
    far_ref,
    lists_ref,
    *rest,
):
    disp_ref, wanted_ref, cross_ref = rest[-3:]
    me = me_ref[0]
    chip, near, diag, far = places(me)
    block = couple_ref.shape[2]
    quarter, eighth = block // 4, block // 8
    pieces = (
        (1, lax.rem(near, 2), near_ref[: 2 * quarter, :]),
        (2, near, near_ref[2 * quarter : 2 * (quarter + eighth), :]),
        (2, diag, diag_ref[: 2 * eighth, :]),
        (2, far, far_ref[...]),
    )
    for columns, value in coupled(pieces, couple_ref):
        disp_ref[:, columns] = (partial_ref[:, columns] + value).astype(BF16)
    tall = 2 * capacity // 128
    tail = list_height(capacity, 2)
    if rides:
        beside = near_ref[2 * (quarter + eighth) :, :128].astype(F32)
        opposite = diag_ref[2 * eighth :, :128].astype(F32)
        low = lax.rem(chip, 2) == 0
        behind, ahead = jnp.where(low, opposite, beside), jnp.where(low, beside, opposite)
    else:
        behind, ahead = rest[0][:, :128].astype(F32), rest[1][:, :128].astype(F32)
    odd = lax.rem(me, 2) == 1
    across = jnp.where(odd, ahead, behind)
    ours = pair_ref[pair_ref.shape[0] - tail :, :128].astype(F32)
    wanted_ref[:, :capacity] = unpacked(behind, 0, capacity)
    wanted_ref[:, capacity : 2 * capacity] = unpacked(ahead, 0, capacity)
    wanted_ref[:, 2 * capacity : 3 * capacity] = unpacked(ours, 0, capacity)
    wanted_ref[:, 3 * capacity :] = unpacked(
        filled(list_rows(lists_ref[...], OWN, capacity), tail), 0, capacity
    )
    cross_ref[...] = gathered(disp_ref, unpacked(across, tall, capacity))


def gather_kernel(capacity, first, disp_ref, wanted_ref, left_ref, right_ref):
    both = gathered(
        disp_ref, wanted_ref[:, first * capacity : (first + 2) * capacity]
    )
    left_ref[...] = both[:, :capacity]
    right_ref[...] = both[:, capacity:]


def permute_kernel(first, key_ref, operators_ref, out_ref):
    clusters, _, rows = operators_ref.shape
    tile = 384
    for part in range(out_ref.shape[0] // tile):
        for cluster in range(clusters):
            for at in range(0, tile, 128):
                pick = one_hot(
                    key_ref[cluster : cluster + 1, :], first + part * tile + at, 128
                )
                moved = jnp.dot(pick, operators_ref[cluster], preferred_element_type=F32)
                start = part * tile + at
                out_ref[start : start + 128, cluster * rows : (cluster + 1) * rows] = (
                    moved.astype(BF16)
                )


def early_kernel(first, key_ref, operators_ref, pair_ref, own_ref, cross_ref, out_ref):
    clusters, _, _ = out_ref.shape
    arrived = jnp.concatenate([pair_ref[...], own_ref[...], cross_ref[...]], axis=1)
    for cluster in range(clusters):
        place = jnp.concatenate(
            [
                one_hot(key_ref[cluster : cluster + 1, :], first + at, 128)
                for at in range(0, arrived.shape[1], 128)
            ],
            axis=0,
        )
        placed = jnp.dot(arrived, place, preferred_element_type=F32).astype(BF16)
        out_ref[cluster] = jnp.dot(
            placed, operators_ref[cluster], preferred_element_type=F32
        )


def late_kernel(
    scale,
    weight_ref,
    compliance_ref,
    early_ref,
    moved_ref,
    plus_ref,
    minus_ref,
    stress_ref,
    energy_ref,
):
    clusters, modes, rows = stress_ref.shape
    points = energy_ref.shape[1]
    weight = jnp.broadcast_to(weight_ref[...], (8, modes)).T[:, :1]
    arrived = jnp.concatenate([plus_ref[...], minus_ref[...]], axis=1)
    late = jnp.dot(arrived, moved_ref[...], preferred_element_type=F32)
    for cluster in range(clusters):
        value = early_ref[cluster] + late[:, cluster * rows : (cluster + 1) * rows]
        stress_ref[cluster] = value
        square = jnp.sum(value * value * weight, axis=0, keepdims=True)
        square = square * compliance_ref[cluster : cluster + 1, :]
        term = square[:, :points]
        for part in range(1, rows // points):
            term = term + square[:, part * points : (part + 1) * points]
        energy_ref[cluster : cluster + 1, :] = term * scale


def store_kernel(source_ref, target_hbm, sem):
    move = pltpu.make_async_copy(source_ref, target_hbm, sem)
    move.start()
    move.wait()


def share_kernel(at_ref, mine_ref, other_ref, out_ref):
    clusters, points = mine_ref.shape
    total = mine_ref[...] + other_ref[...]
    row = [total[c : c + 1, :] for c in range(clusters)]
    lanes = (clusters * points + 127) // 128 * 128
    if lanes > clusters * points:
        row.append(jnp.zeros((1, lanes - clusters * points), F32))
    flat = jnp.broadcast_to(jnp.concatenate(row, axis=1), (8, lanes))
    share = out_ref.shape[1]
    moved = pltpu.roll(flat, lanes - at_ref[0] * share, 1)
    out_ref[...] = moved[0:1, :share]


def shards(
    leaf_coords,
    leaf_modes,
    constraint_modes,
    sep_one,
    sep_two,
    sep_three,
    cluster_rows,
    operators,
    compliance,
    modal_weight,
):
    sub_count = lax.axis_size("sub")
    mode_count = lax.axis_size("mode")
    me = lax.axis_index("sub").astype(I32).reshape(1)
    leaves, modes, _ = leaf_coords.shape
    width = leaf_modes.shape[2]
    dof_count = leaves * width
    clusters, slots = cluster_rows.shape
    rows = operators.shape[2]
    points = rows // 6
    capacity = clusters * slots // 4
    smem = pl.BlockSpec(memory_space=pltpu.SMEM)
    vmem = pl.BlockSpec(memory_space=VMEM)
    hbm = pl.BlockSpec(memory_space=pltpu.HBM)
    array = jax.ShapeDtypeStruct
    half, quarter, eighth = sep_one.shape[1], sep_two.shape[1], sep_three.shape[1]

    tail = list_height(capacity, 2)
    rides = sub_count == 2 * GROUP
    two_t, three_t = sep_two.T, sep_three.T

    tall = (5 * capacity // 128 + 7) // 8 * 8
    key, lists = call(
        lambda *refs: index_kernel(sub_count, dof_count, capacity, *refs),
        (me, cluster_rows),
        (array((clusters, slots), I32), array((2 * tall, 128), F32)),
        8,
        1000000000,
        [smem, vmem],
    )
    held = half + quarter + eighth + tail
    bag = call(
        lambda *refs: pack_kernel(capacity, *refs),
        (sep_one, two_t, three_t, lists),
        array((held, modes), BF16),
        4,
        10000000,
    )
    pair = swap_with(bag, "sub", 1)
    extra = tail if rides else 0
    spare = () if rides else (array((tail, modes), BF16),) * 2
    near, diag, far, *loose = call(
        lambda *refs: relay_kernel(capacity, rides, half, *refs),
        (me, bag, pair, lists),
        (
            array((2 * (quarter + eighth) + extra, modes), BF16),
            array((2 * eighth + extra, modes), BF16),
            array((2 * eighth, modes), BF16),
        )
        + spare,
        4,
        10000000,
        [smem, vmem, vmem, vmem],
    )
    near = swap_with(near, "sub", 2)
    diag = swap_with(diag, "sub", 6)
    far = swap_with(far, "sub", 4)
    if loose:
        loose = [shift_by(loose[0], "sub", 2), shift_by(loose[1], "sub", -2)]
    direct = call(
        direct_kernel, (leaf_coords, leaf_modes), array((modes, dof_count), F32), 4, 1500000000
    )
    partial = call(
        partial_kernel,
        (me, direct, constraint_modes, bag, pair),
        array((modes, dof_count), F32),
        12,
        1500000000,
        [smem] + [vmem] * 4,
    )
    disp, wanted, cross = call(
        lambda *refs: displace_kernel(capacity, rides, *refs),
        (me, partial, constraint_modes, pair, near, diag, far, lists, *loose),
        (
            array((modes, dof_count), BF16),
            array((1, 4 * capacity), I32),
            array((modes, capacity), BF16),
        ),
        12,
        3000000000,
        [smem] + [vmem] * (7 + len(loose)),
    )
    cross = swap_across(cross, "sub")
    flow = array((modes, capacity), BF16)
    plus, minus = call(
        lambda *refs: gather_kernel(capacity, 0, *refs),
        (disp, wanted),
        (flow, flow),
        12,
        2000000000,
    )
    plus = shift_by(plus, "sub", -2)
    minus = shift_by(minus, "sub", 2)
    other, own = call(
        lambda *refs: gather_kernel(capacity, 2, *refs),
        (disp, wanted),
        (flow, flow),
        12,
        2000000000,
    )
    other = swap_with(other, "sub", 1)
    moved_far = call(
        lambda *refs: permute_kernel(0, *refs),
        (key, operators),
        array((2 * capacity, clusters * rows), BF16),
        8,
        2000000000,
    )
    early = call(
        lambda *refs: early_kernel(2 * capacity, *refs),
        (key, operators, other, own, cross),
        array((clusters, modes, rows), F32),
        8,
        500000000,
    )
    stresses, energy = call(
        lambda *refs: late_kernel(0.5 / (modes * mode_count), *refs),
        (modal_weight.reshape(1, modes), compliance, early, moved_far, plus, minus),
        (array((clusters, modes, rows), F32), array((clusters, points), F32)),
        8,
        500000000,
    )
    mask = 1
    while 2 * mask < mode_count:
        energy = energy + swap_with(energy, "mode", mask)
        mask *= 2
    arrived = swap_with(energy, "mode", mask)
    stresses = pl.pallas_call(
        store_kernel,
        out_shape=array((clusters, modes, rows), F32),
        in_specs=[vmem],
        out_specs=hbm,
        scratch_shapes=[pltpu.SemaphoreType.DMA],
        compiler_params=pltpu.CompilerParams(vmem_limit_bytes=4 * 1024 * 1024),
        cost_estimate=pl.CostEstimate(flops=500000000, bytes_accessed=2000000, transcendentals=0),
        name="store",
    )(stresses)
    at = lax.axis_index("mode").astype(I32).reshape(1)
    share = clusters * points // mode_count
    strain_energy = call(
        share_kernel, (at, energy, arrived), array((1, share), F32), 4, 1000, [smem, vmem, vmem]
    )
    return (stresses, strain_energy.reshape(share))


def solution(mesh):
    return jax.shard_map(
        shards,
        mesh=mesh,
        in_specs=(
            P("sub", "mode", None),
            P("sub", None, None),
            P("sub", None, None, None),
            P("mode", "sub"),
            P("mode", "sub"),
            P("mode", "sub"),
            P("sub", None),
            P("sub", None, None),
            P("sub", None),
            P("mode"),
        ),
        out_specs=(P("sub", "mode", None), P(("sub", "mode"))),
        check_vma=False,
    )
```

```python
import jax
import jax.numpy as jnp
from jax import lax
from jax.experimental import pallas as pl
from jax.experimental.pallas import tpu as pltpu
from jax.sharding import PartitionSpec as P


VMEM = pltpu.VMEM
F32 = jnp.float32
BF16 = jnp.bfloat16
I32 = jnp.int32
BASE = 64
GROUP = 4

OUTER, CROSS, PAIR, OWN, NEAR = range(5)


def swap_with(value, axis, mask):
    return lax.ppermute(value, axis, [(i, i ^ mask) for i in range(lax.axis_size(axis))])


def swap_across(value, axis):
    peers = lax.axis_size(axis)
    return lax.ppermute(
        value, axis, [(i, (i + 2 * (i % 2) - 1) % peers) for i in range(peers)]
    )


def swap_outer(value, axis):
    peers = lax.axis_size(axis)
    return lax.ppermute(
        value, axis, [(i, (i + 4 * (i // 2 % 2) - 2) % peers) for i in range(peers)]
    )


def call(kernel, inputs, outputs, mib, flops, specs=None, scratch=()):
    vmem = pl.BlockSpec(memory_space=VMEM)
    many = isinstance(outputs, tuple)
    nbytes = sum(x.size * x.dtype.itemsize for x in inputs)
    return pl.pallas_call(
        kernel,
        out_shape=outputs,
        in_specs=specs or [vmem] * len(inputs),
        out_specs=(vmem,) * len(outputs) if many else vmem,
        scratch_shapes=list(scratch),
        compiler_params=pltpu.CompilerParams(vmem_limit_bytes=mib * 1024 * 1024),
        cost_estimate=pl.CostEstimate(flops=flops, bytes_accessed=nbytes, transcendentals=0),
    )(*inputs)


def one_hot(target, first, rows):
    local = target - first
    local = jnp.where((local >= 0) & (local < rows), local, -1).astype(F32).astype(BF16)
    ids = lax.broadcasted_iota(I32, (rows, target.shape[1]), 0).astype(F32).astype(BF16)
    hit = ids == jnp.broadcast_to(local, ids.shape)
    return jnp.where(hit, jnp.ones((), BF16), jnp.zeros((), BF16))


def list_rows(lists, group, capacity):
    parts = capacity // 128
    low = lists.shape[0] // 2 + group * parts
    return [lists[group * parts : (group + 1) * parts, :], lists[low : low + parts, :]]


def filled(rows, count):
    lanes = rows[0].shape[1]
    rest = count - sum(row.shape[0] for row in rows)
    if not rest:
        return jnp.concatenate(rows, axis=0)
    return jnp.concatenate(rows + [jnp.zeros((rest, lanes), F32)], axis=0)


def unpacked(block, start, capacity):
    parts = capacity // 128
    block = block.astype(F32)
    high = [block[start + i : start + i + 1, :] for i in range(parts)]
    low = [block[start + parts + i : start + parts + i + 1, :] for i in range(parts)]
    wanted = jnp.concatenate(high, axis=1) * float(BASE) + jnp.concatenate(low, axis=1)
    return wanted.astype(I32)


def list_height(capacity, lists):
    return (2 * capacity // 128 * lists + 15) // 16 * 16


def index_kernel(sub_count, dof_count, capacity, me_ref, rows_ref, key_ref, lists_ref):
    clusters, width = rows_ref.shape
    high = (clusters + 7) // 8 * 8
    row = jnp.concatenate(
        [rows_ref[...], jnp.full((high - clusters, width), -1, I32)], axis=0
    )
    before = lax.broadcasted_iota(I32, (width, width), 0)
    after = lax.broadcasted_iota(I32, (width, width), 1)
    upper = jnp.where(before <= after, 1.0, 0.0).astype(BF16)
    me = me_ref[0]
    odd = lax.rem(me, 2)
    source = lax.div(row, jnp.int32(dof_count))
    local = row - source * dof_count
    distance = source - me
    distance = jnp.where(distance < 0, distance + sub_count, distance)
    offset = jnp.where(distance > sub_count // 2, distance - sub_count, distance)
    cross = 2 * odd - 1
    outer = 4 * lax.rem(lax.div(me, 2), 2) - 2
    classes = (outer, cross, -cross, 0, -outer)
    masks = jnp.concatenate(
        [jnp.where((offset == each) & (row >= 0), 1.0, 0.0) for each in classes], axis=0
    )
    counts = jnp.dot(masks.astype(BF16), upper, preferred_element_type=F32)
    key = jnp.zeros((clusters, width), F32)
    for number in range(len(classes)):
        at = number * high
        carried = jnp.full((1, 1), float(number * capacity - 1), F32)
        placed = []
        for cluster in range(clusters):
            count = counts[at + cluster : at + cluster + 1, :]
            placed.append(count + carried)
            carried = carried + count[:, width - 1 : width]
        key = key + masks[at : at + clusters, :] * jnp.concatenate(placed, axis=0)
    key = key.astype(I32)
    key_ref[...] = key
    tall = lists_ref.shape[0] // 2
    rank_high = lax.div(key, jnp.int32(128))
    rank_low = key - rank_high * 128
    digit_high = lax.div(local, jnp.int32(BASE))
    digits = (digit_high.astype(F32), (local - digit_high * BASE).astype(F32))
    ids = lax.broadcasted_iota(I32, (tall, width), 0)
    values, picks = [], []
    for cluster in range(clusters):
        at = slice(cluster, cluster + 1)
        hit = ids == rank_high[at, :]
        values.append(
            jnp.concatenate([jnp.where(hit, digit[at, :], 0.0) for digit in digits], axis=0)
        )
        picks.append(one_hot(rank_low[at, :], 0, 128))
    lists_ref[...] = lax.dot_general(
        jnp.concatenate(values, axis=1).astype(BF16),
        jnp.concatenate(picks, axis=1),
        (((1,), (1,)), ((), ())),
        preferred_element_type=F32,
    )


def pack_kernel(capacity, one_ref, two_ref, three_ref, lists_ref, bag_ref):
    tail = list_height(capacity, 2)
    lists = lists_ref[...]
    at = 0
    for value in (one_ref[...].astype(F32).T.astype(BF16), two_ref[...], three_ref[...]):
        bag_ref[at : at + value.shape[0], :] = value
        at += value.shape[0]
    put_lists(
        bag_ref, at, list_rows(lists, PAIR, capacity) + list_rows(lists, CROSS, capacity), tail
    )


def put_lists(ref, at, rows, tail):
    ref[at : at + tail, :] = jnp.zeros((tail, ref.shape[1]), BF16)
    ref[at : at + tail, :128] = filled(rows, tail).astype(BF16)


def relay_kernel(
    capacity, rides, half, me_ref, bag_ref, pair_ref, lists_ref, near_ref, diag_ref, far_ref, *rest
):
    tail = list_height(capacity, 2)
    tall = 2 * capacity // 128
    quarter, eighth = half // 2, half // 4
    odd = lax.rem(me_ref[0], 2)
    lists = lists_ref[...]
    relayed = pair_ref[half + quarter + eighth :, :128].astype(F32)[tall : 2 * tall, :]
    beside = list_rows(lists, NEAR, capacity) + [relayed]
    opposite = list_rows(lists, OUTER, capacity) + [relayed]

    def put(ref, at, rows, core, value):
        ref[pl.ds(pl.multiple_of(at + core * rows, rows), rows), :] = value

    for core, ref in ((odd, bag_ref), (1 - odd, pair_ref)):
        two = ref[half : half + quarter, :]
        three = ref[half + quarter : half + quarter + eighth, :]
        put(near_ref, 0, quarter, core, two)
        put(near_ref, 2 * quarter, eighth, core, three)
        put(diag_ref, 0, eighth, core, three)
        put(far_ref, 0, eighth, core, three)
    put_lists(near_ref, 2 * (quarter + eighth), beside, tail)
    if rides:
        put_lists(diag_ref, 2 * eighth, opposite, tail)
    else:
        put_lists(rest[0], 0, opposite, tail)


def direct_kernel(coords_ref, modes_ref, out_ref):
    leaves = coords_ref.shape[0]
    width = modes_ref.shape[2]
    for leaf in range(leaves):
        out_ref[:, leaf * width : (leaf + 1) * width] = jnp.dot(
            coords_ref[leaf], modes_ref[leaf], preferred_element_type=F32
        )


def gathered(disp_ref, wanted):
    depth = 256
    total = None
    for at in range(0, disp_ref.shape[1], depth):
        part = jnp.dot(
            disp_ref[:, at : at + depth], one_hot(wanted, at, depth), preferred_element_type=F32
        )
        total = part if total is None else total + part
    return total.astype(BF16)


def coupled(pieces, couple_ref):
    leaves, _, _, width = couple_ref.shape
    anc = jnp.concatenate([value for level, at, value in pieces], axis=0)
    anc = anc.astype(F32).T.astype(BF16)
    for leaf in range(leaves):
        weights = []
        for level, at, value in pieces:
            rows = value.shape[0]
            start = pl.multiple_of(at * rows, rows)
            weights.append(couple_ref[leaf, level, pl.ds(start, rows), :])
        columns = slice(leaf * width, (leaf + 1) * width)
        yield columns, jnp.dot(
            anc, jnp.concatenate(weights, axis=0), preferred_element_type=F32
        )


def places(me):
    chip = lax.rem(lax.div(me, 2), GROUP)
    near = chip + 1 - 2 * lax.rem(chip, 2)
    return chip, near, lax.rem(near + 2, GROUP), lax.rem(chip + 2, GROUP)


def partial_kernel(me_ref, direct_ref, couple_ref, bag_ref, pair_ref, out_ref):
    me = me_ref[0]
    odd = lax.rem(me, 2)
    chip, _, _, _ = places(me)
    block = couple_ref.shape[2]
    half, quarter, eighth = block // 2, block // 4, block // 8
    pieces = []
    for core, ref in ((odd, bag_ref), (1 - odd, pair_ref)):
        pieces += [
            (0, core, ref[:half, :]),
            (1, 2 * lax.rem(chip, 2) + core, ref[half : half + quarter, :]),
            (2, 2 * chip + core, ref[half + quarter : half + quarter + eighth, :]),
        ]
    for columns, value in coupled(pieces, couple_ref):
        out_ref[:, columns] = direct_ref[:, columns] + value


def displace_kernel(
    capacity,
    rides,
    me_ref,
    partial_ref,
    couple_ref,
    pair_ref,
    near_ref,
    diag_ref,
    far_ref,
    lists_ref,
    *rest,
):
    disp_ref, wanted_ref, first_ref = rest[-3:]
    me = me_ref[0]
    chip, near, diag, far = places(me)
    block = couple_ref.shape[2]
    quarter, eighth = block // 4, block // 8
    pieces = (
        (1, lax.rem(near, 2), near_ref[: 2 * quarter, :]),
        (2, near, near_ref[2 * quarter : 2 * (quarter + eighth), :]),
        (2, diag, diag_ref[: 2 * eighth, :]),
        (2, far, far_ref[...]),
    )
    for columns, value in coupled(pieces, couple_ref):
        disp_ref[:, columns] = (partial_ref[:, columns] + value).astype(BF16)
    tall = 2 * capacity // 128
    tail = list_height(capacity, 2)
    beside = near_ref[2 * (quarter + eighth) :, :128].astype(F32)
    opposite = (diag_ref[2 * eighth :, :128] if rides else rest[0][:, :128]).astype(F32)
    odd, high = lax.rem(me, 2), lax.rem(chip, 2)
    across = jnp.where(odd != high, beside, opposite)
    ours = pair_ref[pair_ref.shape[0] - tail :, :128].astype(F32)
    wanted_ref[:, :capacity] = unpacked(opposite, 0, capacity)
    wanted_ref[:, capacity : 2 * capacity] = unpacked(across, tall, capacity)
    wanted_ref[:, 2 * capacity : 3 * capacity] = unpacked(ours, 0, capacity)
    wanted_ref[:, 3 * capacity :] = unpacked(
        filled(list_rows(lists_ref[...], OWN, capacity), tail), 0, capacity
    )
    first_ref[...] = gathered(disp_ref, unpacked(beside, 0, capacity))


def gather_kernel(capacity, first, disp_ref, wanted_ref, left_ref, right_ref):
    both = gathered(
        disp_ref, wanted_ref[:, first * capacity : (first + 2) * capacity]
    )
    left_ref[...] = both[:, :capacity]
    right_ref[...] = both[:, capacity:]


def permute_kernel(first, key_ref, operators_ref, out_ref):
    clusters, _, rows = operators_ref.shape
    tile = 384
    for part in range(out_ref.shape[0] // tile):
        for cluster in range(clusters):
            for at in range(0, tile, 128):
                pick = one_hot(
                    key_ref[cluster : cluster + 1, :], first + part * tile + at, 128
                )
                moved = jnp.dot(pick, operators_ref[cluster], preferred_element_type=F32)
                start = part * tile + at
                out_ref[start : start + 128, cluster * rows : (cluster + 1) * rows] = (
                    moved.astype(BF16)
                )


def early_kernel(first, key_ref, operators_ref, pair_ref, own_ref, near_ref, out_ref):
    clusters, _, _ = out_ref.shape
    arrived = jnp.concatenate([pair_ref[...], own_ref[...], near_ref[...]], axis=1)
    for cluster in range(clusters):
        place = jnp.concatenate(
            [
                one_hot(key_ref[cluster : cluster + 1, :], first + at, 128)
                for at in range(0, arrived.shape[1], 128)
            ],
            axis=0,
        )
        placed = jnp.dot(arrived, place, preferred_element_type=F32).astype(BF16)
        out_ref[cluster] = jnp.dot(
            placed, operators_ref[cluster], preferred_element_type=F32
        )


def late_kernel(
    scale,
    weight_ref,
    compliance_ref,
    early_ref,
    moved_ref,
    outer_ref,
    cross_ref,
    stress_ref,
    energy_ref,
):
    clusters, modes, rows = stress_ref.shape
    points = energy_ref.shape[1]
    weight = jnp.broadcast_to(weight_ref[...], (8, modes)).T[:, :1]
    arrived = jnp.concatenate([outer_ref[...], cross_ref[...]], axis=1)
    late = jnp.dot(arrived, moved_ref[...], preferred_element_type=F32)
    for cluster in range(clusters):
        value = early_ref[cluster] + late[:, cluster * rows : (cluster + 1) * rows]
        stress_ref[cluster] = value
        square = jnp.sum(value * value * weight, axis=0, keepdims=True)
        square = square * compliance_ref[cluster : cluster + 1, :]
        term = square[:, :points]
        for part in range(1, rows // points):
            term = term + square[:, part * points : (part + 1) * points]
        energy_ref[cluster : cluster + 1, :] = term * scale


def store_kernel(source_ref, target_hbm, sem):
    move = pltpu.make_async_copy(source_ref, target_hbm, sem)
    move.start()
    move.wait()


def share_kernel(at_ref, mine_ref, other_ref, out_ref):
    clusters, points = mine_ref.shape
    total = mine_ref[...] + other_ref[...]
    row = [total[c : c + 1, :] for c in range(clusters)]
    lanes = (clusters * points + 127) // 128 * 128
    if lanes > clusters * points:
        row.append(jnp.zeros((1, lanes - clusters * points), F32))
    flat = jnp.broadcast_to(jnp.concatenate(row, axis=1), (8, lanes))
    share = out_ref.shape[1]
    moved = pltpu.roll(flat, lanes - at_ref[0] * share, 1)
    out_ref[...] = moved[0:1, :share]


def shards(
    leaf_coords,
    leaf_modes,
    constraint_modes,
    sep_one,
    sep_two,
    sep_three,
    cluster_rows,
    operators,
    compliance,
    modal_weight,
):
    sub_count = lax.axis_size("sub")
    mode_count = lax.axis_size("mode")
    me = lax.axis_index("sub").astype(I32).reshape(1)
    leaves, modes, _ = leaf_coords.shape
    width = leaf_modes.shape[2]
    dof_count = leaves * width
    clusters, slots = cluster_rows.shape
    rows = operators.shape[2]
    points = rows // 6
    capacity = clusters * slots // 4
    smem = pl.BlockSpec(memory_space=pltpu.SMEM)
    vmem = pl.BlockSpec(memory_space=VMEM)
    hbm = pl.BlockSpec(memory_space=pltpu.HBM)
    array = jax.ShapeDtypeStruct
    half, quarter, eighth = sep_one.shape[1], sep_two.shape[1], sep_three.shape[1]

    tail = list_height(capacity, 2)
    rides = sub_count == 2 * GROUP
    two_t, three_t = sep_two.T, sep_three.T

    tall = (5 * capacity // 128 + 7) // 8 * 8
    key, lists = call(
        lambda *refs: index_kernel(sub_count, dof_count, capacity, *refs),
        (me, cluster_rows),
        (array((clusters, slots), I32), array((2 * tall, 128), F32)),
        8,
        1000000000,
        [smem, vmem],
    )
    held = half + quarter + eighth + tail
    bag = call(
        lambda *refs: pack_kernel(capacity, *refs),
        (sep_one, two_t, three_t, lists),
        array((held, modes), BF16),
        4,
        10000000,
    )
    pair = swap_with(bag, "sub", 1)
    extra = tail if rides else 0
    spare = () if rides else (array((tail, modes), BF16),)
    near, diag, far, *loose = call(
        lambda *refs: relay_kernel(capacity, rides, half, *refs),
        (me, bag, pair, lists),
        (
            array((2 * (quarter + eighth) + tail, modes), BF16),
            array((2 * eighth + extra, modes), BF16),
            array((2 * eighth, modes), BF16),
        )
        + spare,
        4,
        10000000,
        [smem, vmem, vmem, vmem],
    )
    near = swap_with(near, "sub", 2)
    diag = swap_with(diag, "sub", 6)
    far = swap_with(far, "sub", 4)
    loose = [swap_outer(value, "sub") for value in loose]
    direct = call(
        direct_kernel, (leaf_coords, leaf_modes), array((modes, dof_count), F32), 4, 1500000000
    )
    partial = call(
        partial_kernel,
        (me, direct, constraint_modes, bag, pair),
        array((modes, dof_count), F32),
        12,
        1500000000,
        [smem] + [vmem] * 4,
    )
    disp, wanted, beside = call(
        lambda *refs: displace_kernel(capacity, rides, *refs),
        (me, partial, constraint_modes, pair, near, diag, far, lists, *loose),
        (
            array((modes, dof_count), BF16),
            array((1, 4 * capacity), I32),
            array((modes, capacity), BF16),
        ),
        12,
        3000000000,
        [smem] + [vmem] * (7 + len(loose)),
    )
    beside = swap_with(beside, "sub", 2)
    flow = array((modes, capacity), BF16)
    outer, cross = call(
        lambda *refs: gather_kernel(capacity, 0, *refs),
        (disp, wanted),
        (flow, flow),
        12,
        2000000000,
    )
    outer = swap_outer(outer, "sub")
    cross = swap_across(cross, "sub")
    other, own = call(
        lambda *refs: gather_kernel(capacity, 2, *refs),
        (disp, wanted),
        (flow, flow),
        12,
        2000000000,
    )
    other = swap_with(other, "sub", 1)
    moved_far = call(
        lambda *refs: permute_kernel(0, *refs),
        (key, operators),
        array((2 * capacity, clusters * rows), BF16),
        8,
        2000000000,
    )
    early = call(
        lambda *refs: early_kernel(2 * capacity, *refs),
        (key, operators, other, own, beside),
        array((clusters, modes, rows), F32),
        8,
        500000000,
    )
    stresses, energy = call(
        lambda *refs: late_kernel(0.5 / (modes * mode_count), *refs),
        (modal_weight.reshape(1, modes), compliance, early, moved_far, outer, cross),
        (array((clusters, modes, rows), F32), array((clusters, points), F32)),
        8,
        500000000,
    )
    mask = 1
    while 2 * mask < mode_count:
        energy = energy + swap_with(energy, "mode", mask)
        mask *= 2
    arrived = swap_with(energy, "mode", mask)
    stresses = pl.pallas_call(
        store_kernel,
        out_shape=array((clusters, modes, rows), F32),
        in_specs=[vmem],
        out_specs=hbm,
        scratch_shapes=[pltpu.SemaphoreType.DMA],
        compiler_params=pltpu.CompilerParams(vmem_limit_bytes=4 * 1024 * 1024),
        cost_estimate=pl.CostEstimate(flops=500000000, bytes_accessed=2000000, transcendentals=0),
        name="store",
    )(stresses)
    at = lax.axis_index("mode").astype(I32).reshape(1)
    share = clusters * points // mode_count
    strain_energy = call(
        share_kernel, (at, energy, arrived), array((1, share), F32), 4, 1000, [smem, vmem, vmem]
    )
    return (stresses, strain_energy.reshape(share))


def solution(mesh):
    return jax.shard_map(
        shards,
        mesh=mesh,
        in_specs=(
            P("sub", "mode", None),
            P("sub", None, None),
            P("sub", None, None, None),
            P("mode", "sub"),
            P("mode", "sub"),
            P("mode", "sub"),
            P("sub", None),
            P("sub", None, None),
            P("sub", None),
            P("mode"),
        ),
        out_specs=(P("sub", "mode", None), P(("sub", "mode"))),
        check_vma=False,
    )
```

```python
import jax
import jax.numpy as jnp
from jax import lax
from jax.experimental import pallas as pl
from jax.experimental.pallas import tpu as pltpu
from jax.sharding import PartitionSpec as P


VMEM = pltpu.VMEM
F32 = jnp.float32
BF16 = jnp.bfloat16
I32 = jnp.int32
BASE = 64
GROUP = 4

OUTER, CROSS, PAIR, OWN, NEAR = range(5)


def swap_with(value, axis, mask):
    return lax.ppermute(value, axis, [(i, i ^ mask) for i in range(lax.axis_size(axis))])


def swap_across(value, axis):
    peers = lax.axis_size(axis)
    return lax.ppermute(
        value, axis, [(i, (i + 2 * (i % 2) - 1) % peers) for i in range(peers)]
    )


def swap_outer(value, axis):
    peers = lax.axis_size(axis)
    return lax.ppermute(
        value, axis, [(i, (i + 4 * (i // 2 % 2) - 2) % peers) for i in range(peers)]
    )


def call(kernel, inputs, outputs, mib, flops, specs=None, scratch=()):
    vmem = pl.BlockSpec(memory_space=VMEM)
    many = isinstance(outputs, tuple)
    nbytes = sum(x.size * x.dtype.itemsize for x in inputs)
    return pl.pallas_call(
        kernel,
        out_shape=outputs,
        in_specs=specs or [vmem] * len(inputs),
        out_specs=(vmem,) * len(outputs) if many else vmem,
        scratch_shapes=list(scratch),
        compiler_params=pltpu.CompilerParams(vmem_limit_bytes=mib * 1024 * 1024),
        cost_estimate=pl.CostEstimate(flops=flops, bytes_accessed=nbytes, transcendentals=0),
    )(*inputs)


def one_hot(target, first, rows):
    local = target - first
    local = jnp.where((local >= 0) & (local < rows), local, -1).astype(F32).astype(BF16)
    ids = lax.broadcasted_iota(I32, (rows, target.shape[1]), 0).astype(F32).astype(BF16)
    hit = ids == jnp.broadcast_to(local, ids.shape)
    return jnp.where(hit, jnp.ones((), BF16), jnp.zeros((), BF16))


def list_rows(lists, group, capacity):
    parts = capacity // 128
    low = lists.shape[0] // 2 + group * parts
    return [lists[group * parts : (group + 1) * parts, :], lists[low : low + parts, :]]


def filled(rows, count):
    lanes = rows[0].shape[1]
    rest = count - sum(row.shape[0] for row in rows)
    if not rest:
        return jnp.concatenate(rows, axis=0)
    return jnp.concatenate(rows + [jnp.zeros((rest, lanes), F32)], axis=0)


def unpacked(block, start, capacity):
    parts = capacity // 128
    block = block.astype(F32)
    high = [block[start + i : start + i + 1, :] for i in range(parts)]
    low = [block[start + parts + i : start + parts + i + 1, :] for i in range(parts)]
    wanted = jnp.concatenate(high, axis=1) * float(BASE) + jnp.concatenate(low, axis=1)
    return wanted.astype(I32)


def list_height(capacity, lists):
    return (2 * capacity // 128 * lists + 15) // 16 * 16


def index_kernel(sub_count, dof_count, capacity, me_ref, rows_ref, key_ref, lists_ref):
    clusters, width = rows_ref.shape
    high = (clusters + 7) // 8 * 8
    row = jnp.concatenate(
        [rows_ref[...], jnp.full((high - clusters, width), -1, I32)], axis=0
    )
    before = lax.broadcasted_iota(I32, (width, width), 0)
    after = lax.broadcasted_iota(I32, (width, width), 1)
    upper = jnp.where(before <= after, 1.0, 0.0).astype(BF16)
    me = me_ref[0]
    odd = lax.rem(me, 2)
    source = lax.div(row, jnp.int32(dof_count))
    local = row - source * dof_count
    distance = source - me
    distance = jnp.where(distance < 0, distance + sub_count, distance)
    offset = jnp.where(distance > sub_count // 2, distance - sub_count, distance)
    cross = 2 * odd - 1
    outer = 4 * lax.rem(lax.div(me, 2), 2) - 2
    classes = (outer, cross, -cross, 0, -outer)
    masks = jnp.concatenate(
        [jnp.where((offset == each) & (row >= 0), 1.0, 0.0) for each in classes], axis=0
    )
    counts = jnp.dot(masks.astype(BF16), upper, preferred_element_type=F32)
    key = jnp.zeros((clusters, width), F32)
    for number in range(len(classes)):
        at = number * high
        carried = jnp.full((1, 1), float(number * capacity - 1), F32)
        placed = []
        for cluster in range(clusters):
            count = counts[at + cluster : at + cluster + 1, :]
            placed.append(count + carried)
            carried = carried + count[:, width - 1 : width]
        key = key + masks[at : at + clusters, :] * jnp.concatenate(placed, axis=0)
    key = key.astype(I32)
    key_ref[...] = key
    tall = lists_ref.shape[0] // 2
    rank_high = lax.div(key, jnp.int32(128))
    rank_low = key - rank_high * 128
    digit_high = lax.div(local, jnp.int32(BASE))
    digits = (digit_high.astype(F32), (local - digit_high * BASE).astype(F32))
    ids = lax.broadcasted_iota(I32, (tall, width), 0)
    values, picks = [], []
    for cluster in range(clusters):
        at = slice(cluster, cluster + 1)
        hit = ids == rank_high[at, :]
        values.append(
            jnp.concatenate([jnp.where(hit, digit[at, :], 0.0) for digit in digits], axis=0)
        )
        picks.append(one_hot(rank_low[at, :], 0, 128))
    lists_ref[...] = lax.dot_general(
        jnp.concatenate(values, axis=1).astype(BF16),
        jnp.concatenate(picks, axis=1),
        (((1,), (1,)), ((), ())),
        preferred_element_type=F32,
    )


def pack_kernel(capacity, one_ref, two_ref, three_ref, lists_ref, bag_ref):
    tail = list_height(capacity, 2)
    lists = lists_ref[...]
    at = 0
    for value in (one_ref[...].astype(F32).T.astype(BF16), two_ref[...], three_ref[...]):
        bag_ref[at : at + value.shape[0], :] = value
        at += value.shape[0]
    put_lists(
        bag_ref, at, list_rows(lists, PAIR, capacity) + list_rows(lists, CROSS, capacity), tail
    )


def put_lists(ref, at, rows, tail):
    ref[at : at + tail, :] = jnp.zeros((tail, ref.shape[1]), BF16)
    ref[at : at + tail, :128] = filled(rows, tail).astype(BF16)


def relay_kernel(
    capacity, rides, half, me_ref, bag_ref, pair_ref, lists_ref, near_ref, diag_ref, far_ref, *rest
):
    tail = list_height(capacity, 2)
    tall = 2 * capacity // 128
    quarter, eighth = half // 2, half // 4
    odd = lax.rem(me_ref[0], 2)
    lists = lists_ref[...]
    relayed = pair_ref[half + quarter + eighth :, :128].astype(F32)[tall : 2 * tall, :]
    beside = list_rows(lists, NEAR, capacity) + [relayed]
    opposite = list_rows(lists, OUTER, capacity) + [relayed]

    def put(ref, at, rows, core, value):
        ref[pl.ds(pl.multiple_of(at + core * rows, rows), rows), :] = value

    for core, ref in ((odd, bag_ref), (1 - odd, pair_ref)):
        two = ref[half : half + quarter, :]
        three = ref[half + quarter : half + quarter + eighth, :]
        put(near_ref, 0, quarter, core, two)
        put(near_ref, 2 * quarter, eighth, core, three)
        put(diag_ref, 0, eighth, core, three)
        put(far_ref, 0, eighth, core, three)
    put_lists(near_ref, 2 * (quarter + eighth), beside, tail)
    if rides:
        put_lists(diag_ref, 2 * eighth, opposite, tail)
    else:
        put_lists(rest[0], 0, opposite, tail)


def direct_kernel(coords_ref, modes_ref, out_ref):
    leaves = coords_ref.shape[0]
    width = modes_ref.shape[2]
    for leaf in range(leaves):
        out_ref[:, leaf * width : (leaf + 1) * width] = jnp.dot(
            coords_ref[leaf], modes_ref[leaf], preferred_element_type=F32
        )


def gathered(disp_ref, wanted):
    depth = 256
    total = None
    for at in range(0, disp_ref.shape[1], depth):
        part = jnp.dot(
            disp_ref[:, at : at + depth], one_hot(wanted, at, depth), preferred_element_type=F32
        )
        total = part if total is None else total + part
    return total.astype(BF16)


def coupled(pieces, couple_ref):
    leaves, _, _, width = couple_ref.shape
    anc = jnp.concatenate([value for level, at, value in pieces], axis=0)
    anc = anc.astype(F32).T.astype(BF16)
    for leaf in range(leaves):
        weights = []
        for level, at, value in pieces:
            rows = value.shape[0]
            start = pl.multiple_of(at * rows, rows)
            weights.append(couple_ref[leaf, level, pl.ds(start, rows), :])
        columns = slice(leaf * width, (leaf + 1) * width)
        yield columns, jnp.dot(
            anc, jnp.concatenate(weights, axis=0), preferred_element_type=F32
        )


def places(me):
    chip = lax.rem(lax.div(me, 2), GROUP)
    near = chip + 1 - 2 * lax.rem(chip, 2)
    return chip, near, lax.rem(near + 2, GROUP), lax.rem(chip + 2, GROUP)


def partial_kernel(me_ref, direct_ref, couple_ref, bag_ref, pair_ref, out_ref):
    me = me_ref[0]
    odd = lax.rem(me, 2)
    chip, _, _, _ = places(me)
    block = couple_ref.shape[2]
    half, quarter, eighth = block // 2, block // 4, block // 8
    pieces = []
    for core, ref in ((odd, bag_ref), (1 - odd, pair_ref)):
        pieces += [
            (0, core, ref[:half, :]),
            (1, 2 * lax.rem(chip, 2) + core, ref[half : half + quarter, :]),
            (2, 2 * chip + core, ref[half + quarter : half + quarter + eighth, :]),
        ]
    for columns, value in coupled(pieces, couple_ref):
        out_ref[:, columns] = direct_ref[:, columns] + value


def near_kernel(me_ref, partial_ref, couple_ref, near_ref, out_ref):
    _, near, _, _ = places(me_ref[0])
    block = couple_ref.shape[2]
    quarter, eighth = block // 4, block // 8
    pieces = (
        (1, lax.rem(near, 2), near_ref[: 2 * quarter, :]),
        (2, near, near_ref[2 * quarter : 2 * (quarter + eighth), :]),
    )
    for columns, value in coupled(pieces, couple_ref):
        out_ref[:, columns] = partial_ref[:, columns] + value


def displace_kernel(
    capacity,
    rides,
    me_ref,
    partial_ref,
    couple_ref,
    pair_ref,
    near_ref,
    diag_ref,
    far_ref,
    lists_ref,
    *rest,
):
    disp_ref, wanted_ref, first_ref = rest[-3:]
    me = me_ref[0]
    chip, _, diag, far = places(me)
    block = couple_ref.shape[2]
    quarter, eighth = block // 4, block // 8
    pieces = ((2, diag, diag_ref[: 2 * eighth, :]), (2, far, far_ref[...]))
    for columns, value in coupled(pieces, couple_ref):
        disp_ref[:, columns] = (partial_ref[:, columns] + value).astype(BF16)
    tall = 2 * capacity // 128
    tail = list_height(capacity, 2)
    beside = near_ref[2 * (quarter + eighth) :, :128].astype(F32)
    opposite = (diag_ref[2 * eighth :, :128] if rides else rest[0][:, :128]).astype(F32)
    odd, high = lax.rem(me, 2), lax.rem(chip, 2)
    across = jnp.where(odd != high, beside, opposite)
    ours = pair_ref[pair_ref.shape[0] - tail :, :128].astype(F32)
    wanted_ref[:, :capacity] = unpacked(opposite, 0, capacity)
    wanted_ref[:, capacity : 2 * capacity] = unpacked(across, tall, capacity)
    wanted_ref[:, 2 * capacity : 3 * capacity] = unpacked(ours, 0, capacity)
    wanted_ref[:, 3 * capacity :] = unpacked(
        filled(list_rows(lists_ref[...], OWN, capacity), tail), 0, capacity
    )
    first_ref[...] = gathered(disp_ref, unpacked(beside, 0, capacity))


def gather_kernel(capacity, first, disp_ref, wanted_ref, left_ref, right_ref):
    both = gathered(
        disp_ref, wanted_ref[:, first * capacity : (first + 2) * capacity]
    )
    left_ref[...] = both[:, :capacity]
    right_ref[...] = both[:, capacity:]


def permute_kernel(first, key_ref, operators_ref, out_ref):
    clusters, _, rows = operators_ref.shape
    tile = 384
    for part in range(out_ref.shape[0] // tile):
        for cluster in range(clusters):
            for at in range(0, tile, 128):
                pick = one_hot(
                    key_ref[cluster : cluster + 1, :], first + part * tile + at, 128
                )
                moved = jnp.dot(pick, operators_ref[cluster], preferred_element_type=F32)
                start = part * tile + at
                out_ref[start : start + 128, cluster * rows : (cluster + 1) * rows] = (
                    moved.astype(BF16)
                )


def early_kernel(first, key_ref, operators_ref, pair_ref, own_ref, near_ref, out_ref):
    clusters, _, _ = out_ref.shape
    arrived = jnp.concatenate([pair_ref[...], own_ref[...], near_ref[...]], axis=1)
    for cluster in range(clusters):
        place = jnp.concatenate(
            [
                one_hot(key_ref[cluster : cluster + 1, :], first + at, 128)
                for at in range(0, arrived.shape[1], 128)
            ],
            axis=0,
        )
        placed = jnp.dot(arrived, place, preferred_element_type=F32).astype(BF16)
        out_ref[cluster] = jnp.dot(
            placed, operators_ref[cluster], preferred_element_type=F32
        )


def late_kernel(
    scale,
    weight_ref,
    compliance_ref,
    early_ref,
    moved_ref,
    outer_ref,
    cross_ref,
    stress_ref,
    energy_ref,
):
    clusters, modes, rows = stress_ref.shape
    points = energy_ref.shape[1]
    weight = jnp.broadcast_to(weight_ref[...], (8, modes)).T[:, :1]
    arrived = jnp.concatenate([outer_ref[...], cross_ref[...]], axis=1)
    late = jnp.dot(arrived, moved_ref[...], preferred_element_type=F32)
    for cluster in range(clusters):
        value = early_ref[cluster] + late[:, cluster * rows : (cluster + 1) * rows]
        stress_ref[cluster] = value
        square = jnp.sum(value * value * weight, axis=0, keepdims=True)
        square = square * compliance_ref[cluster : cluster + 1, :]
        term = square[:, :points]
        for part in range(1, rows // points):
            term = term + square[:, part * points : (part + 1) * points]
        energy_ref[cluster : cluster + 1, :] = term * scale


def store_kernel(source_ref, target_hbm, sem):
    move = pltpu.make_async_copy(source_ref, target_hbm, sem)
    move.start()
    move.wait()


def share_kernel(at_ref, mine_ref, other_ref, out_ref):
    clusters, points = mine_ref.shape
    total = mine_ref[...] + other_ref[...]
    row = [total[c : c + 1, :] for c in range(clusters)]
    lanes = (clusters * points + 127) // 128 * 128
    if lanes > clusters * points:
        row.append(jnp.zeros((1, lanes - clusters * points), F32))
    flat = jnp.broadcast_to(jnp.concatenate(row, axis=1), (8, lanes))
    share = out_ref.shape[1]
    moved = pltpu.roll(flat, lax.rem(lanes - at_ref[0] * share, lanes), 1)
    out_ref[...] = moved[0:1, :share]


def shards(
    leaf_coords,
    leaf_modes,
    constraint_modes,
    sep_one,
    sep_two,
    sep_three,
    cluster_rows,
    operators,
    compliance,
    modal_weight,
):
    sub_count = lax.axis_size("sub")
    mode_count = lax.axis_size("mode")
    me = lax.axis_index("sub").astype(I32).reshape(1)
    leaves, modes, _ = leaf_coords.shape
    width = leaf_modes.shape[2]
    dof_count = leaves * width
    clusters, slots = cluster_rows.shape
    rows = operators.shape[2]
    points = rows // 6
    capacity = clusters * slots // 4
    smem = pl.BlockSpec(memory_space=pltpu.SMEM)
    vmem = pl.BlockSpec(memory_space=VMEM)
    hbm = pl.BlockSpec(memory_space=pltpu.HBM)
    array = jax.ShapeDtypeStruct
    half, quarter, eighth = sep_one.shape[1], sep_two.shape[1], sep_three.shape[1]

    tail = list_height(capacity, 2)
    rides = sub_count == 2 * GROUP
    two_t, three_t = sep_two.T, sep_three.T

    tall = (5 * capacity // 128 + 7) // 8 * 8
    key, lists = call(
        lambda *refs: index_kernel(sub_count, dof_count, capacity, *refs),
        (me, cluster_rows),
        (array((clusters, slots), I32), array((2 * tall, 128), F32)),
        8,
        1000000000,
        [smem, vmem],
    )
    held = half + quarter + eighth + tail
    bag = call(
        lambda *refs: pack_kernel(capacity, *refs),
        (sep_one, two_t, three_t, lists),
        array((held, modes), BF16),
        4,
        10000000,
    )
    pair = swap_with(bag, "sub", 1)
    extra = tail if rides else 0
    spare = () if rides else (array((tail, modes), BF16),)
    near, diag, far, *loose = call(
        lambda *refs: relay_kernel(capacity, rides, half, *refs),
        (me, bag, pair, lists),
        (
            array((2 * (quarter + eighth) + tail, modes), BF16),
            array((2 * eighth + extra, modes), BF16),
            array((2 * eighth, modes), BF16),
        )
        + spare,
        4,
        10000000,
        [smem, vmem, vmem, vmem],
    )
    near = swap_with(near, "sub", 2)
    diag = swap_with(diag, "sub", 6)
    far = swap_with(far, "sub", 4)
    loose = [swap_outer(value, "sub") for value in loose]
    direct = call(
        direct_kernel, (leaf_coords, leaf_modes), array((modes, dof_count), F32), 4, 1500000000
    )
    partial = call(
        partial_kernel,
        (me, direct, constraint_modes, bag, pair),
        array((modes, dof_count), F32),
        12,
        1500000000,
        [smem] + [vmem] * 4,
    )
    partial = call(
        near_kernel,
        (me, partial, constraint_modes, near),
        array((modes, dof_count), F32),
        8,
        700000000,
        [smem] + [vmem] * 3,
    )
    disp, wanted, beside = call(
        lambda *refs: displace_kernel(capacity, rides, *refs),
        (me, partial, constraint_modes, pair, near, diag, far, lists, *loose),
        (
            array((modes, dof_count), BF16),
            array((1, 4 * capacity), I32),
            array((modes, capacity), BF16),
        ),
        12,
        3000000000,
        [smem] + [vmem] * (7 + len(loose)),
    )
    beside = swap_with(beside, "sub", 2)
    flow = array((modes, capacity), BF16)
    outer, cross = call(
        lambda *refs: gather_kernel(capacity, 0, *refs),
        (disp, wanted),
        (flow, flow),
        12,
        2000000000,
    )
    outer = swap_outer(outer, "sub")
    cross = swap_across(cross, "sub")
    other, own = call(
        lambda *refs: gather_kernel(capacity, 2, *refs),
        (disp, wanted),
        (flow, flow),
        12,
        2000000000,
    )
    other = swap_with(other, "sub", 1)
    moved_far = call(
        lambda *refs: permute_kernel(0, *refs),
        (key, operators),
        array((2 * capacity, clusters * rows), BF16),
        8,
        2000000000,
    )
    early = call(
        lambda *refs: early_kernel(2 * capacity, *refs),
        (key, operators, other, own, beside),
        array((clusters, modes, rows), F32),
        8,
        500000000,
    )
    stresses, energy = call(
        lambda *refs: late_kernel(0.5 / (modes * mode_count), *refs),
        (modal_weight.reshape(1, modes), compliance, early, moved_far, outer, cross),
        (array((clusters, modes, rows), F32), array((clusters, points), F32)),
        8,
        500000000,
    )
    mask = 1
    while 2 * mask < mode_count:
        energy = energy + swap_with(energy, "mode", mask)
        mask *= 2
    arrived = swap_with(energy, "mode", mask)
    stresses = pl.pallas_call(
        store_kernel,
        out_shape=array((clusters, modes, rows), F32),
        in_specs=[vmem],
        out_specs=hbm,
        scratch_shapes=[pltpu.SemaphoreType.DMA],
        compiler_params=pltpu.CompilerParams(vmem_limit_bytes=4 * 1024 * 1024),
        cost_estimate=pl.CostEstimate(flops=500000000, bytes_accessed=2000000, transcendentals=0),
        name="store",
    )(stresses)
    at = lax.axis_index("mode").astype(I32).reshape(1)
    share = clusters * points // mode_count
    strain_energy = call(
        share_kernel, (at, energy, arrived), array((1, share), F32), 4, 1000, [smem, vmem, vmem]
    )
    return (stresses, strain_energy.reshape(share))


def solution(mesh):
    return jax.shard_map(
        shards,
        mesh=mesh,
        in_specs=(
            P("sub", "mode", None),
            P("sub", None, None),
            P("sub", None, None, None),
            P("mode", "sub"),
            P("mode", "sub"),
            P("mode", "sub"),
            P("sub", None),
            P("sub", None, None),
            P("sub", None),
            P("mode"),
        ),
        out_specs=(P("sub", "mode", None), P(("sub", "mode"))),
        check_vma=False,
    )
```
